128 devices in a mesh: lon: 8 (over z, y_hi), lat: 16 (over y_lo, x, core).
Axes of the slice: x: 4, y: 4 (y_hi: 2, y_lo: 2; y = y_hi * 2 + y_lo), z: 4, core: 2. Of those that a mesh axis runs over, the one named last changes fastest.
Arguments:
- fields: float32 [4, 8, 1024, 3600], P(None, None, 'lat', 'lon'), may hold values from -6 to 6
- thickness: float32 [8], replicated, may hold values from 5 to 250
- cutoff: int32 [256], replicated, may hold values from 2 to 1800
- barotropic: float32 [3, 1024, 3600], P(None, 'lat', 'lon'), may hold values from -6 to 6
- land_sea: int32 [1024, 3600], P('lat', 'lon'), may hold values 0 or 1
Outputs:
- filtered_tracers: float32 [2, 8, 1024, 3600], P(None, None, 'lat', 'lon')
- velocity: float32 [2, 8, 1024, 3600], P(None, None, 'lat', 'lon')
- sea_level: float32 [1024, 3600], P('lat', 'lon')
The draws below stay inside these ranges and needn't reach their ends.
Inputs may be any that keep to these rules, and one draw needn't show every extreme that they name: `cutoff`: each filtered row's highest kept wavenumber.
All inputs are finite; a program needn't handle non-finite values. No bound on the sum of `land_sea` on one device may be relied on, other than what follows from the above.
Results may differ from the reference program's by a relative error of at most 0.0003.
Values sent between devices are 32-bit elements; how exact they have to be, the bound alone decides.
No kernel may reach another device: no remote copies, remote signals or barrier semaphores. Data moves between devices by JAX's collectives and lax.ppermute only.
A program may use at most 128 MiB of HBM per device.

```python
import math
import jax
import jax.numpy as jnp
from jax import lax

NLON = 3600
LEV = 8
SUB = 20
NLAT = 1024
NPOLE = 128


def touch_ends(drawn, own_key, smallest, largest):
    extent = drawn.shape
    index_at = [jax.random.randint(jax.random.fold_in(own_key, axis), (), 0, extent[axis]) for axis in range(len(extent))]
    drawn = drawn.at[tuple(index_at)].set(smallest)
    longest = extent.index(max(extent))
    index_at[longest] = (index_at[longest] + 1) % extent[longest]
    return drawn.at[tuple(index_at)].set(largest)


def shard_levels(own_key, dims, split, least, top_value):
    def one(dim, shards_of):
        heights = jax.random.uniform(jax.random.fold_in(jax.random.fold_in(own_key, 6), dim), (shards_of,), jnp.float32, least / len(split), top_value / len(split))
        return jnp.repeat(jnp.exp(heights), dims[dim] // shards_of).reshape((-1,) + (1,) * (len(dims) - dim - 1))

    level = one(*split[0])
    for cut in split[1:]:
        level = level * one(*cut)
    return level


def gaussian(rng, dims, scale, most, shards=(), kind=jnp.bfloat16):
    drawn = scale * jax.random.normal(rng, dims, jnp.float32)
    if shards:
        drawn = drawn * shard_levels(rng, dims, shards, -0.22, 0.18)
    return jnp.clip(drawn, -most, most).astype(kind)


def setup_inputs(seed: int = 0) -> dict:
    arg_keys = jax.random.split(jax.random.key(seed), 6)
    fields = gaussian(arg_keys[0], (4, LEV, NLAT, NLON), 1.0, 6.0, ((2, 16), (3, 8)), jnp.float32)
    thickness = jnp.clip(jnp.exp(jax.random.uniform(arg_keys[1], (LEV,), jnp.float32, math.log(5.0), math.log(250.0))), 5.0, 250.0)
    cutoff = touch_ends(jax.random.randint(arg_keys[2], (2 * NPOLE,), 2, NLON // 2 + 1), jax.random.fold_in(arg_keys[2], 1), 2, (NLON // 2 + 1) - 1).astype(jnp.int32)
    barotropic = gaussian(arg_keys[3], (3, NLAT, NLON), 1.0, 6.0, ((1, 16), (2, 8)), jnp.float32)
    land_sea = touch_ends((jax.random.randint(arg_keys[4], (NLAT, NLON), 0, 5) < 4).astype(jnp.int32), jax.random.fold_in(arg_keys[4], 1), 0, 1)
    return {"fields": fields, "thickness": thickness, "cutoff": cutoff, "barotropic": barotropic, "land_sea": land_sea}


wave_coef = 0.65


def polar_filter(values, row_cuts):
    circle_len = values.shape[-1]
    spectrum = jnp.fft.rfft(values, axis=-1)
    wavenumber = jnp.arange(circle_len // 2 + 1)
    kept_mask = wavenumber[None, :] <= row_cuts[:, None]
    return jnp.fft.irfft(spectrum * kept_mask, n=circle_len, axis=-1).astype(values.dtype)


def reference(fields, thickness, cutoff, barotropic, land_sea):
    total_rows = fields.shape[2]
    pole_rows = cutoff.shape[0] // 2
    north_rows = polar_filter(fields[:, :, :pole_rows], cutoff[:pole_rows])
    south_rows = polar_filter(fields[:, :, total_rows - pole_rows:], cutoff[pole_rows:])
    filtered = jnp.concatenate([north_rows, fields[:, :, pole_rows:total_rows - pole_rows], south_rows], axis=2)
    ocean_cell = land_sea.astype(fields.dtype)
    row_number = jnp.arange(total_rows)
    east_open = ocean_cell * jnp.roll(ocean_cell, -1, 1)
    north_open = ocean_cell * jnp.roll(ocean_cell, -1, 0) * (row_number != total_rows - 1).astype(fields.dtype)[:, None]
    surface = barotropic[0]
    eastward = barotropic[1] * east_open
    northward = barotropic[2] * north_open
    for subcycle in range(SUB):
        divergence = eastward - jnp.roll(eastward, 1, 1) + northward - jnp.roll(northward, 1, 0)
        surface = surface - wave_coef * ocean_cell * divergence
        eastward = east_open * (eastward - wave_coef * (jnp.roll(surface, -1, 1) - surface))
        northward = north_open * (northward - wave_coef * (jnp.roll(surface, -1, 0) - surface))
    weights = thickness / jnp.sum(thickness)
    currents = filtered[2:]
    column = jnp.einsum("k,ckij->cij", weights, currents, precision=lax.Precision.HIGHEST)
    velocity = jnp.stack([east_open, north_open])[:, None] * (currents - column[:, None] + jnp.stack([eastward, northward])[:, None])
    return filtered[:2], velocity, surface
```

```python
import math
import numpy as np
import jax
import jax.numpy as jnp
from jax import lax
from jax.experimental import pallas as pl
from jax.experimental.pallas import tpu as pltpu
from jax.sharding import PartitionSpec as P

WAVE = 0.65
SUB = 20
RIM = 21
ROWH = 24
SEG = 225
KPAD = 256
MROW = 232


def cplx_add(a, b):
    return (a[0] + b[0], (b[1] if a[1] is None else a[1] if b[1] is None else a[1] + b[1]))


def cplx_sub(a, b):
    if b[1] is None:
        im = a[1]
    elif a[1] is None:
        im = -b[1]
    else:
        im = a[1] - b[1]
    return (a[0] - b[0], im)


def conj(a):
    return (a[0], None if a[1] is None else -a[1])


def turn(a, num, den):
    num %= den
    if num == 0:
        return a
    c, s = math.cos(2 * math.pi * num / den), math.sin(2 * math.pi * num / den)
    re, im = a
    if (4 * num) % den == 0:
        q = 4 * num // den
        if q == 1:
            return (jnp.zeros_like(re) if im is None else -im, re)
        if q == 2:
            return (-re, None if im is None else -im)
        return (jnp.zeros_like(re) if im is None else im, -re)
    if im is None:
        return (re * c, re * s)
    if abs(abs(c) - abs(s)) < 1e-12:
        h = abs(c)
        sc, ss = math.copysign(1.0, c), math.copysign(1.0, s)
        x = re if sc > 0 else -re
        y = im if ss > 0 else -im
        x2 = re if ss > 0 else -re
        y2 = im if sc > 0 else -im
        return ((x - y) * h, (x2 + y2) * h)
    return (re * c - im * s, re * s + im * c)


def real_dft(xs):
    n = len(xs)
    if n == 2:
        return [(xs[0] + xs[1], None), (xs[0] - xs[1], None)]
    even, odd = real_dft(xs[0::2]), real_dft(xs[1::2])
    out = [None] * (n // 2 + 1)
    for r in range(n // 4 + 1):
        o = turn(odd[r], -r, n)
        out[r] = cplx_add(even[r], o)
        if r != n // 2 - r:
            out[n // 2 - r] = conj(cplx_sub(even[r], o))
    return out


def real_idft(ys):
    n = 2 * (len(ys) - 1)
    if n == 2:
        return [ys[0][0] + ys[1][0], ys[0][0] - ys[1][0]]
    even, odd = [], []
    for r in range(n // 4 + 1):
        a, b = ys[r], conj(ys[n // 2 - r])
        if r in (0,):
            a, b = (a[0], None), (b[0], None)
        if r == n // 4:
            even.append((a[0] + a[0], None))
            o = turn((a[0] - a[0], a[1] + a[1]), r, n) if False else None
            odd.append((-(a[1] + a[1]), None))
            continue
        even.append(cplx_add(a, b))
        odd.append(turn(cplx_sub(a, b), r, n))
    e, o = real_idft(even), real_idft(odd)
    out = [None] * n
    out[0::2], out[1::2] = e, o
    return out


def fft_tables():
    k = np.arange(SEG)
    ang = 2.0 * np.pi * ((k[:, None] * k[None, :]) % SEG) / SEG
    w = np.zeros((2 * MROW, KPAD), np.float32)
    w[:SEG, :SEG] = np.cos(ang) / 60.0
    w[MROW : MROW + SEG, :SEG] = np.sin(ang) / 60.0
    tw = np.zeros((MROW, 16), np.float32)
    for r in range(1, 9):
        a = 2.0 * np.pi * r * k / 3600.0
        tw[:SEG, r - 1] = np.cos(a)
        tw[:SEG, r + 7] = np.sin(a)
    return w, tw


def split(x):
    hi = x.astype(jnp.bfloat16)
    lo = (x - hi.astype(jnp.float32)).astype(jnp.bfloat16)
    return hi, lo


def filter_kernel(polar_ref, x_ref, cut_ref, wh_ref, wl_ref, tw_ref, y_ref, r_scr):
    polar = polar_ref[0] != 0
    lanes = x_ref.shape[2]
    two = 2 * lanes

    @pl.when(jnp.logical_not(polar))
    def _():
        y_ref[...] = x_ref[...]

    @pl.when(polar)
    def _():
        r_scr[MROW - 8 :, :] = jnp.zeros((KPAD - MROW + 8, 9 * two), jnp.float32)
        r_scr[:, lanes:two] = jnp.zeros((KPAD, lanes), jnp.float32)
        blocks = [(8 * i, 8) for i in range(SEG // 8)] + [(SEG - 1, 1)]
        for at, rows in blocks:
            xs = []
            for s in range(16):
                d, h = divmod(s, 2)
                xs.append(x_ref[d, pl.ds(h * SEG + at, rows), :])
            zs = real_dft(xs)
            tw = tw_ref[pl.ds(at, rows), :]
            r_scr[pl.ds(at, rows), 0:lanes] = zs[0][0]
            for r in range(1, 9):
                c = jnp.broadcast_to(tw[:, r - 1 : r], (rows, lanes))
                sn = jnp.broadcast_to(tw[:, r + 7 : r + 8], (rows, lanes))
                re, im = zs[r]
                if im is None:
                    ure, uim = re * c, -(re * sn)
                else:
                    ure, uim = re * c + im * sn, im * c - re * sn
                r_scr[pl.ds(at, rows), r * two : r * two + lanes] = ure
                r_scr[pl.ds(at, rows), r * two + lanes : (r + 1) * two] = uim
        cut = jnp.broadcast_to(cut_ref[...], (MROW, lanes))
        kk = lax.broadcasted_iota(jnp.int32, (MROW, lanes), 0) * 16

        def product(x):
            hi, lo = split(x)
            wh, wl = wh_ref[...], wl_ref[...]
            f = lambda a, b: jnp.dot(a, b, preferred_element_type=jnp.float32)
            return f(wh, hi) + f(wl, hi) + f(wh, lo)

        def one_bin(r, carry):
            col = pl.ds(pl.multiple_of(r * two, two), two)
            a = product(r_scr[:, col])
            top, low = a[:MROW], a[MROW:]
            m = kk + r
            keep = jnp.minimum(m, 3600 - m) <= cut
            gre = jnp.where(keep, top[:, :lanes] + low[:, lanes:], 0.0)
            gim = jnp.where(keep, top[:, lanes:] - low[:, :lanes], 0.0)
            r_scr[0:MROW, col] = jnp.concatenate([gre, gim], axis=1)
            b = product(r_scr[:, col])
            top, low = b[:MROW], b[MROW:]
            vre = top[:, :lanes] - low[:, lanes:]
            vim = top[:, lanes:] + low[:, :lanes]
            r_scr[0:MROW, col] = jnp.concatenate([vre, vim], axis=1)
            return carry

        lax.fori_loop(0, 9, one_bin, 0)
        for at, rows in blocks:
            tw = tw_ref[pl.ds(at, rows), :]
            ws = [(r_scr[pl.ds(at, rows), 0:lanes], None)]
            for r in range(1, 9):
                c = jnp.broadcast_to(tw[:, r - 1 : r], (rows, lanes))
                sn = jnp.broadcast_to(tw[:, r + 7 : r + 8], (rows, lanes))
                vre = r_scr[pl.ds(at, rows), r * two : r * two + lanes]
                vim = r_scr[pl.ds(at, rows), r * two + lanes : (r + 1) * two]
                if r == 8:
                    ws.append((vre * c - vim * sn, None))
                else:
                    ws.append((vre * c - vim * sn, vre * sn + vim * c))
            ys = real_idft(ws)
            for s in range(16):
                d, h = divmod(s, 2)
                y_ref[d, pl.ds(h * SEG + at, rows), :] = ys[s]


def filter_call(polar, x, cut, wh, wl, tw):
    lanes = x.shape[2]
    vm = pl.BlockSpec(memory_space=pltpu.VMEM)
    return pl.pallas_call(
        filter_kernel,
        out_shape=jax.ShapeDtypeStruct(x.shape, jnp.float32),
        in_specs=[pl.BlockSpec(memory_space=pltpu.SMEM)] + [vm] * 5,
        out_specs=vm,
        scratch_shapes=[pltpu.VMEM((KPAD, 9 * 2 * lanes), jnp.float32)],
        name="polar_filter",
        compiler_params=pltpu.CompilerParams(vmem_limit_bytes=40 * 1024 * 1024),
    )(polar, x, cut, wh, wl, tw)

ROWS = 64
COLS = 450
LANES = 512
FAR = 112


def lane_ids(rows):
    return lax.broadcasted_iota(jnp.int32, (rows, 128), 1)


def rim_kernel(flow_ref, land_ref, rim_ref, scr):
    lane = lane_ids(ROWS)
    for a in range(4):
        if a < 3:
            scr[:, 0:COLS] = flow_ref[a]
        else:
            scr[:, 0:COLS] = land_ref[...].astype(jnp.float32)
        first = pltpu.roll(scr[:, 0:128], COLS - 384, 1)
        last = pltpu.roll(scr[:, 384:512], LANES - COLS, 1)
        rim_ref[a] = jnp.where(lane < 96, first, last)


def join_kernel(flow_ref, land_ref, east_ref, west_ref, mid_ref, top_ref, low_ref):
    lane = lane_ids(ROWS)
    for a in range(4):
        if a < 3:
            mid_ref[a, :, 0:COLS] = flow_ref[a]
        else:
            mid_ref[a, :, 0:COLS] = land_ref[...].astype(jnp.float32)
        own = mid_ref[a, :, 384:512]
        west = jnp.where(lane >= 128 - RIM, west_ref[a], 0.0)
        east = jnp.where(lane < COLS - 384 + RIM, east_ref[a], west)
        mid_ref[a, :, 384:512] = jnp.where(lane < COLS - 384, own, east)
        top_ref[a] = mid_ref[a, 0:ROWH]
        low_ref[a] = mid_ref[a, ROWS - ROWH :]


def step_kernel(at_ref, mid_ref, top_ref, low_ref, out_ref, s_scr, e_scr, n_scr, oc_scr, eo_scr, no_scr):
    first_row = at_ref[0] * ROWS - ROWH
    total = at_ref[1]
    for a, scr in enumerate((s_scr, e_scr, n_scr, oc_scr)):
        scr[0:8] = jnp.zeros((8, LANES), jnp.float32)
        scr[8 + FAR :] = jnp.zeros((8, LANES), jnp.float32)
        scr[8 : 8 + ROWH] = top_ref[a]
        scr[8 + ROWH : 8 + ROWH + ROWS] = mid_ref[a]
        scr[8 + ROWH + ROWS : 8 + FAR] = low_ref[a]
    for b in range(FAR // 8):
        at = 8 + 8 * b
        oc = oc_scr[at : at + 8]
        row = first_row + 8 * b + lax.broadcasted_iota(jnp.int32, (8, LANES), 0)
        last = (row == total - 1) | (row == -1)
        eo = oc * pltpu.roll(oc, LANES - 1, 1)
        no = jnp.where(last, 0.0, oc * oc_scr[at + 1 : at + 9])
        eo_scr[at : at + 8] = eo
        no_scr[at : at + 8] = no
        e_scr[at : at + 8] = e_scr[at : at + 8] * eo
        n_scr[at : at + 8] = n_scr[at : at + 8] * no

    def step(_, carry):
        for b in range(FAR // 8):
            at = 8 + 8 * b
            e = e_scr[at : at + 8]
            div = e - pltpu.roll(e, 1, 1) + n_scr[at : at + 8] - n_scr[at - 1 : at + 7]
            s_scr[at : at + 8] = s_scr[at : at + 8] - WAVE * oc_scr[at : at + 8] * div
        for b in range(FAR // 8):
            at = 8 + 8 * b
            s = s_scr[at : at + 8]
            e_scr[at : at + 8] = eo_scr[at : at + 8] * (
                e_scr[at : at + 8] - WAVE * (pltpu.roll(s, LANES - 1, 1) - s)
            )
            n_scr[at : at + 8] = no_scr[at : at + 8] * (
                n_scr[at : at + 8] - WAVE * (s_scr[at + 1 : at + 9] - s)
            )
        return carry

    lax.fori_loop(0, SUB, step, 0)
    mine = slice(8 + ROWH, 8 + ROWH + ROWS)
    for a, scr in enumerate((s_scr, e_scr, n_scr, eo_scr, no_scr)):
        out_ref[a] = scr[mine, 0:COLS]


def vm():
    return pl.BlockSpec(memory_space=pltpu.VMEM)


def sm():
    return pl.BlockSpec(memory_space=pltpu.SMEM)


def f32(*dims):
    return jax.ShapeDtypeStruct(dims, jnp.float32)


def barotropic_steps(flow, land, lat_index, total_rows, shift):
    rim = pl.pallas_call(
        rim_kernel,
        out_shape=f32(4, ROWS, 128),
        in_specs=[vm(), vm()],
        out_specs=vm(),
        scratch_shapes=[pltpu.VMEM((ROWS, LANES), jnp.float32)],
        name="rim_columns",
    )(flow, land)
    east = shift(rim, "lon", -1)
    west = shift(rim, "lon", 1)
    mid, top, low = pl.pallas_call(
        join_kernel,
        out_shape=(f32(4, ROWS, LANES), f32(4, ROWH, LANES), f32(4, ROWH, LANES)),
        in_specs=[vm()] * 4,
        out_specs=(vm(), vm(), vm()),
        name="join_columns",
    )(flow, land, east, west)
    above = shift(low, "lat", 1)
    below = shift(top, "lat", -1)
    where = jnp.stack([lat_index, jnp.int32(total_rows)])
    return pl.pallas_call(
        step_kernel,
        out_shape=f32(5, ROWS, COLS),
        in_specs=[sm()] + [vm()] * 3,
        out_specs=vm(),
        scratch_shapes=[pltpu.VMEM((FAR + 16, LANES), jnp.float32)] * 6,
        name="subcycles",
    )(where, mid, above, below)


def shift(value, axis, by):
    size = lax.axis_size(axis)
    return lax.ppermute(value, axis, [(i, (i + by) % size) for i in range(size)])


def body(fields, thickness, cutoff, barotropic, land_sea):
    lon_count = lax.axis_size("lon")
    lat_count = lax.axis_size("lat")
    lat = lax.axis_index("lat")
    components, levels, band_rows, tile_cols = fields.shape
    total_rows = band_rows * lat_count
    pole_rows = cutoff.shape[0] // 2
    pole_bands = pole_rows // band_rows
    polar = (lat < pole_bands) | (lat >= lat_count - pole_bands)
    table, twist = fft_tables()
    table = jnp.asarray(table)
    table_hi, table_lo = split(table)
    twist = jnp.asarray(twist)
    at = jnp.where(lat < pole_bands, lat * band_rows, lat * band_rows - (total_rows - 2 * pole_rows))
    cuts = lax.dynamic_slice_in_dim(cutoff, jnp.clip(at, 0, 2 * pole_rows - band_rows), band_rows)
    per = 2 * levels // lon_count
    cuts = jnp.tile(cuts, per)[None, :]
    flag = polar.astype(jnp.int32)[None]

    def send(pair):
        parts = pair.reshape(lon_count, per * band_rows, tile_cols)
        return lax.all_to_all(parts, "lon", split_axis=0, concat_axis=0)

    def filtered(parts):
        got = filter_call(flag, jnp.swapaxes(parts, 1, 2), cuts, table_hi, table_lo, twist)
        return jnp.swapaxes(got, 1, 2)

    def back(parts):
        got = lax.all_to_all(parts, "lon", split_axis=0, concat_axis=0)
        return got.reshape(2, levels, band_rows, tile_cols)

    flow_parts = send(fields[2:])
    tracer_parts = send(fields[:2])
    new = barotropic_steps(barotropic, land_sea, lat, total_rows, shift)
    currents = back(filtered(flow_parts))
    tracers = back(filtered(tracer_parts))
    weights = thickness / jnp.sum(thickness)
    column = jnp.sum(weights[None, :, None, None] * currents, axis=1)
    velocity = new[3:5][:, None] * (currents - column[:, None] + new[1:3][:, None])
    return (tracers, velocity, new[0])


def solution(mesh):
    return jax.shard_map(
        body,
        mesh=mesh,
        in_specs=(P(None, None, "lat", "lon"), P(), P(), P(None, "lat", "lon"), P("lat", "lon")),
        out_specs=(P(None, None, "lat", "lon"), P(None, None, "lat", "lon"), P("lat", "lon")),
        check_vma=False,
    )
```

```python
import math
import numpy as np
import jax
import jax.numpy as jnp
from jax import lax
from jax.experimental import pallas as pl
from jax.experimental.pallas import tpu as pltpu
from jax.sharding import PartitionSpec as P

WAVE = 0.65
SUB = 20
MIB = 1 << 20
RIM = 21
ROWH = 24
SEG = 225
KPAD = 256
MROW = 232


def cplx_add(a, b):
    return (a[0] + b[0], (b[1] if a[1] is None else a[1] if b[1] is None else a[1] + b[1]))


def cplx_sub(a, b):
    if b[1] is None:
        im = a[1]
    elif a[1] is None:
        im = -b[1]
    else:
        im = a[1] - b[1]
    return (a[0] - b[0], im)


def conj(a):
    return (a[0], None if a[1] is None else -a[1])


def turn(a, num, den):
    num %= den
    if num == 0:
        return a
    c, s = math.cos(2 * math.pi * num / den), math.sin(2 * math.pi * num / den)
    re, im = a
    if (4 * num) % den == 0:
        q = 4 * num // den
        if q == 1:
            return (jnp.zeros_like(re) if im is None else -im, re)
        if q == 2:
            return (-re, None if im is None else -im)
        return (jnp.zeros_like(re) if im is None else im, -re)
    if im is None:
        return (re * c, re * s)
    if abs(abs(c) - abs(s)) < 1e-12:
        h = abs(c)
        sc, ss = math.copysign(1.0, c), math.copysign(1.0, s)
        x = re if sc > 0 else -re
        y = im if ss > 0 else -im
        x2 = re if ss > 0 else -re
        y2 = im if sc > 0 else -im
        return ((x - y) * h, (x2 + y2) * h)
    return (re * c - im * s, re * s + im * c)


def real_dft(xs):
    n = len(xs)
    if n == 2:
        return [(xs[0] + xs[1], None), (xs[0] - xs[1], None)]
    even, odd = real_dft(xs[0::2]), real_dft(xs[1::2])
    out = [None] * (n // 2 + 1)
    for r in range(n // 4 + 1):
        o = turn(odd[r], -r, n)
        out[r] = cplx_add(even[r], o)
        if r != n // 2 - r:
            out[n // 2 - r] = conj(cplx_sub(even[r], o))
    return out


def real_idft(ys):
    n = 2 * (len(ys) - 1)
    if n == 2:
        return [ys[0][0] + ys[1][0], ys[0][0] - ys[1][0]]
    even, odd = [], []
    for r in range(n // 4 + 1):
        a, b = ys[r], conj(ys[n // 2 - r])
        if r in (0,):
            a, b = (a[0], None), (b[0], None)
        if r == n // 4:
            even.append((a[0] + a[0], None))
            o = turn((a[0] - a[0], a[1] + a[1]), r, n) if False else None
            odd.append((-(a[1] + a[1]), None))
            continue
        even.append(cplx_add(a, b))
        odd.append(turn(cplx_sub(a, b), r, n))
    e, o = real_idft(even), real_idft(odd)
    out = [None] * n
    out[0::2], out[1::2] = e, o
    return out


def fft_tables():
    k = np.arange(SEG)
    ang = 2.0 * np.pi * ((k[:, None] * k[None, :]) % SEG) / SEG
    w = np.zeros((2 * MROW, KPAD), np.float32)
    w[:SEG, :SEG] = np.cos(ang) / 60.0
    w[MROW : MROW + SEG, :SEG] = np.sin(ang) / 60.0
    tw = np.zeros((MROW, 16), np.float32)
    for r in range(1, 9):
        a = 2.0 * np.pi * r * k / 3600.0
        tw[:SEG, r - 1] = np.cos(a)
        tw[:SEG, r + 7] = np.sin(a)
    return w, tw


def split(x):
    hi = x.astype(jnp.bfloat16)
    lo = (x - hi.astype(jnp.float32)).astype(jnp.bfloat16)
    return hi, lo


def filter_kernel(
    polar_ref, x_hbm, cut_ref, wh_ref, wl_ref, tw_ref, y_hbm, x_ref, r_scr, in_sem, out_sem
):
    polar = polar_ref[0] != 0
    y_ref = x_ref
    lanes = x_ref.shape[2]
    groups = [pl.ds(128 * g, 128) for g in range(lanes // 128)]

    def get(g):
        at = (slice(None), slice(None), groups[g])
        return pltpu.make_async_copy(x_hbm.at[at], x_ref.at[at], in_sem.at[g])

    def put(g):
        at = (slice(None), slice(None), groups[g])
        return pltpu.make_async_copy(y_ref.at[at], y_hbm.at[at], out_sem.at[g])

    for g in range(lanes // 128):
        get(g).start()
    two = 2 * lanes

    @pl.when(jnp.logical_not(polar))
    def _():
        for g in range(lanes // 128):
            get(g).wait()
            put(g).start()

    @pl.when(polar)
    def _():
        r_scr[MROW - 8 :, :] = jnp.zeros((KPAD - MROW + 8, 9 * two), jnp.float32)
        r_scr[:, lanes:two] = jnp.zeros((KPAD, lanes), jnp.float32)
        blocks = [(8 * i, 8) for i in range(SEG // 8)] + [(SEG - 1, 1)]

        def forward(g):
            lane = groups[g]
            get(g).wait()
            for at, rows in blocks:
                zs = real_dft([x_ref[s // 2, pl.ds(s % 2 * SEG + at, rows), lane] for s in range(16)])
                tw = tw_ref[pl.ds(at, rows), :]
                for r in range(9):
                    re, im = zs[r]
                    if r > 0:
                        c = jnp.broadcast_to(tw[:, r - 1 : r], (rows, 128))
                        sn = jnp.broadcast_to(tw[:, r + 7 : r + 8], (rows, 128))
                        if im is None:
                            re, im = re * c, -(re * sn)
                        else:
                            re, im = re * c + im * sn, im * c - re * sn
                        col = r * two + lanes + g * 128
                        r_scr[pl.ds(at, rows), pl.ds(col, 128)] = im
                    col = r * two + g * 128
                    r_scr[pl.ds(at, rows), pl.ds(col, 128)] = re

        for g in range(lanes // 128):
            forward(g)
        cut = jnp.broadcast_to(cut_ref[...], (MROW, lanes))
        kk = lax.broadcasted_iota(jnp.int32, (MROW, lanes), 0) * 16

        def product(x):
            hi, lo = split(x)
            wh, wl = wh_ref[...], wl_ref[...]
            f = lambda a, b: jnp.dot(a, b, preferred_element_type=jnp.float32)
            return f(wh, hi) + f(wl, hi) + f(wh, lo)

        def one_bin(r, carry):
            col = pl.ds(pl.multiple_of(r * two, two), two)
            a = product(r_scr[:, col])
            top, low = a[:MROW], a[MROW:]
            m = kk + r
            keep = jnp.minimum(m, 3600 - m) <= cut
            gre = jnp.where(keep, top[:, :lanes] + low[:, lanes:], 0.0)
            gim = jnp.where(keep, top[:, lanes:] - low[:, :lanes], 0.0)
            r_scr[0:MROW, col] = jnp.concatenate([gre, gim], axis=1)
            b = product(r_scr[:, col])
            top, low = b[:MROW], b[MROW:]
            vre = top[:, :lanes] - low[:, lanes:]
            vim = top[:, lanes:] + low[:, :lanes]
            r_scr[0:MROW, col] = jnp.concatenate([vre, vim], axis=1)
            return carry

        lax.fori_loop(0, 9, one_bin, 0)

        def inverse(g):
            lane = groups[g]
            for at, rows in blocks:
                tw = tw_ref[pl.ds(at, rows), :]
                ws = []
                for r in range(9):
                    col = r * two + g * 128
                    vre = r_scr[pl.ds(at, rows), pl.ds(col, 128)]
                    if r == 0:
                        ws.append((vre, None))
                        continue
                    col = r * two + lanes + g * 128
                    vim = r_scr[pl.ds(at, rows), pl.ds(col, 128)]
                    c = jnp.broadcast_to(tw[:, r - 1 : r], (rows, 128))
                    sn = jnp.broadcast_to(tw[:, r + 7 : r + 8], (rows, 128))
                    ws.append((vre * c - vim * sn, None if r == 8 else vre * sn + vim * c))
                ys = real_idft(ws)
                for s in range(16):
                    y_ref[s // 2, pl.ds(s % 2 * SEG + at, rows), lane] = ys[s]
            put(g).start()

        for g in range(lanes // 128):
            inverse(g)

    for g in range(lanes // 128):
        put(g).wait()


def filter_call(polar, x, cut, wh, wl, tw):
    lanes = x.shape[2]
    vmem = pl.BlockSpec(memory_space=pltpu.VMEM)
    far = pl.BlockSpec(memory_space=pltpu.HBM)
    dma = pltpu.SemaphoreType.DMA((lanes // 128,))
    return pl.pallas_call(
        filter_kernel,
        out_shape=pltpu.HBM(x.shape, jnp.float32),
        in_specs=[pl.BlockSpec(memory_space=pltpu.SMEM), far] + [vmem] * 4,
        out_specs=far,
        scratch_shapes=[
            pltpu.VMEM(x.shape, jnp.float32),
            pltpu.VMEM((KPAD, 9 * 2 * lanes), jnp.float32),
            dma,
            dma,
        ],
        name="polar_filter",
        compiler_params=pltpu.CompilerParams(vmem_limit_bytes=32 * MIB),
    )(polar, x, cut, wh, wl, tw)


ROWS = 64
COLS = 450
LANES = 512
FAR = 112


def lane_ids(rows):
    return lax.broadcasted_iota(jnp.int32, (rows, 128), 1)


def rim_kernel(flow_ref, land_ref, rim_ref, scr):
    lane = lane_ids(ROWS)
    for a in range(4):
        if a < 3:
            scr[:, 0:COLS] = flow_ref[a]
        else:
            scr[:, 0:COLS] = land_ref[...].astype(jnp.float32)
        first = pltpu.roll(scr[:, 0:128], COLS - 384, 1)
        last = pltpu.roll(scr[:, 384:512], LANES - COLS, 1)
        rim_ref[a] = jnp.where(lane < 96, first, last)


def join_kernel(flow_ref, land_ref, east_ref, west_ref, mid_ref, top_ref, low_ref):
    lane = lane_ids(ROWS)
    for a in range(4):
        if a < 3:
            mid_ref[a, :, 0:COLS] = flow_ref[a]
        else:
            mid_ref[a, :, 0:COLS] = land_ref[...].astype(jnp.float32)
        own = mid_ref[a, :, 384:512]
        west = jnp.where(lane >= 128 - RIM, west_ref[a], 0.0)
        east = jnp.where(lane < COLS - 384 + RIM, east_ref[a], west)
        mid_ref[a, :, 384:512] = jnp.where(lane < COLS - 384, own, east)
        top_ref[a] = mid_ref[a, 0:ROWH]
        low_ref[a] = mid_ref[a, ROWS - ROWH :]


def step_kernel(at_ref, mid_ref, top_ref, low_ref, out_ref, sea_ref, s_scr, e_scr, n_scr, oc_scr, eo_scr, no_scr):
    first_row = at_ref[0] * ROWS - ROWH
    total = at_ref[1]
    for a, scr in enumerate((s_scr, e_scr, n_scr, oc_scr)):
        scr[0:8] = jnp.zeros((8, LANES), jnp.float32)
        scr[8 + FAR :] = jnp.zeros((8, LANES), jnp.float32)
        scr[8 : 8 + ROWH] = top_ref[a]
        scr[8 + ROWH : 8 + ROWH + ROWS] = mid_ref[a]
        scr[8 + ROWH + ROWS : 8 + FAR] = low_ref[a]
    for b in range(FAR // 8):
        at = 8 + 8 * b
        oc = oc_scr[at : at + 8]
        row = first_row + 8 * b + lax.broadcasted_iota(jnp.int32, (8, LANES), 0)
        last = (row == total - 1) | (row == -1)
        eo = oc * pltpu.roll(oc, LANES - 1, 1)
        no = jnp.where(last, 0.0, oc * oc_scr[at + 1 : at + 9])
        eo_scr[at : at + 8] = eo
        no_scr[at : at + 8] = no
        e_scr[at : at + 8] = e_scr[at : at + 8] * eo
        n_scr[at : at + 8] = n_scr[at : at + 8] * no

    def step(_, carry):
        for b in range(FAR // 8):
            at = 8 + 8 * b
            e = e_scr[at : at + 8]
            div = e - pltpu.roll(e, 1, 1) + n_scr[at : at + 8] - n_scr[at - 1 : at + 7]
            s_scr[at : at + 8] = s_scr[at : at + 8] - WAVE * oc_scr[at : at + 8] * div
        for b in range(FAR // 8):
            at = 8 + 8 * b
            s = s_scr[at : at + 8]
            e_scr[at : at + 8] = eo_scr[at : at + 8] * (
                e_scr[at : at + 8] - WAVE * (pltpu.roll(s, LANES - 1, 1) - s)
            )
            n_scr[at : at + 8] = no_scr[at : at + 8] * (
                n_scr[at : at + 8] - WAVE * (s_scr[at + 1 : at + 9] - s)
            )
        return carry

    lax.fori_loop(0, SUB, step, 0)
    mine = slice(8 + ROWH, 8 + ROWH + ROWS)
    sea_ref[...] = s_scr[mine, 0:COLS]
    for a, scr in enumerate((e_scr, n_scr, eo_scr, no_scr)):
        out_ref[a] = scr[mine, 0:COLS]


def vm():
    return pl.BlockSpec(memory_space=pltpu.VMEM)


def hbm():
    return pl.BlockSpec(memory_space=pltpu.HBM)


def sm():
    return pl.BlockSpec(memory_space=pltpu.SMEM)


def f32(*dims):
    return jax.ShapeDtypeStruct(dims, jnp.float32)


def barotropic_rims(flow, land, shift):
    rim = pl.pallas_call(
        rim_kernel,
        out_shape=f32(4, ROWS, 128),
        in_specs=[vm(), vm()],
        out_specs=vm(),
        scratch_shapes=[pltpu.VMEM((ROWS, LANES), jnp.float32)],
        name="rim_columns",
        compiler_params=pltpu.CompilerParams(vmem_limit_bytes=8 * MIB),
    )(flow, land)
    east = shift(rim, "lon", -1)
    west = shift(rim, "lon", 1)
    return east, west


def barotropic_steps(flow, land, east, west, lat_index, total_rows, shift):
    mid, top, low = pl.pallas_call(
        join_kernel,
        out_shape=(f32(4, ROWS, LANES), f32(4, ROWH, LANES), f32(4, ROWH, LANES)),
        in_specs=[vm()] * 4,
        out_specs=(vm(), vm(), vm()),
        name="join_columns",
        compiler_params=pltpu.CompilerParams(vmem_limit_bytes=8 * MIB),
    )(flow, land, east, west)
    above = shift(low, "lat", 1)
    below = shift(top, "lat", -1)
    where = jnp.stack([lat_index, jnp.int32(total_rows)])
    return pl.pallas_call(
        step_kernel,
        out_shape=(f32(4, ROWS, COLS), f32(ROWS, COLS)),
        in_specs=[sm()] + [vm()] * 3,
        out_specs=(vm(), vm()),
        scratch_shapes=[pltpu.VMEM((FAR + 16, LANES), jnp.float32)] * 6,
        name="subcycles",
        compiler_params=pltpu.CompilerParams(vmem_limit_bytes=8 * MIB),
    )(where, mid, above, below)


def pack_kernel(thick_ref, x_hbm, out_hbm, x_scr, y_scr, in_sem, out_sem):
    parts = out_hbm.shape[0]
    per = x_hbm.shape[0] // parts
    levels = thick_ref.shape[0]
    tracer_parts = parts // 2
    gets = []
    for p in range(parts):
        span = pl.ds(p * per, per)
        gets.append(pltpu.make_async_copy(x_hbm.at[span], x_scr.at[span], in_sem.at[p]))
        gets[-1].start()
    puts = []

    def put(p, xs):
        y_scr[p] = jnp.concatenate(xs, axis=0).T
        puts.append(pltpu.make_async_copy(y_scr.at[p], out_hbm.at[p], out_sem.at[p]))
        puts[-1].start()

    for p in range(tracer_parts):
        gets[p].wait()
        put(p, [x_scr[p * per + i] for i in range(per)])
    whole = thick_ref[0]
    for k in range(1, levels):
        whole = whole + thick_ref[k]
    scale = 1.0 / jnp.full((1, COLS), whole, jnp.float32)
    group = levels // per
    for p in range(tracer_parts, parts, group):
        for q in range(group):
            gets[p + q].wait()
        mean = thick_ref[0] * x_scr[p * per]
        for k in range(1, levels):
            mean = mean + thick_ref[k] * x_scr[p * per + k]
        mean = mean * scale
        for q in range(group):
            put(p + q, [x_scr[(p + q) * per + i] - mean for i in range(per)])
    for copy in puts:
        copy.wait()


def unpack_kernel(got_hbm, new_ref, tracer_hbm, speed_hbm, x_scr, y_scr, in_sem, out_sem):
    parts = got_hbm.shape[0]
    held = parts // 2
    per = tracer_hbm.shape[0] // held
    gets, puts = [], []
    for p in range(parts):
        gets.append(pltpu.make_async_copy(got_hbm.at[p], x_scr.at[p], in_sem.at[p]))
        gets[-1].start()
    for p in range(parts):
        gets[p].wait()
        block = x_scr[p].T
        for k in range(per):
            piece = block[k * ROWS : (k + 1) * ROWS]
            if p >= held:
                field = (p - held) // (held // 2)
                piece = new_ref[2 + field] * (piece + new_ref[field])
            y_scr[p, k] = piece
        to = tracer_hbm if p < held else speed_hbm
        span = pl.ds(p % held * per, per)
        puts.append(pltpu.make_async_copy(y_scr.at[p], to.at[span], out_sem.at[p]))
        puts[-1].start()
    for copy in puts:
        copy.wait()


def shift(value, axis, by):
    size = lax.axis_size(axis)
    return lax.ppermute(value, axis, [(i, (i + by) % size) for i in range(size)])


def body(fields, thickness, cutoff, barotropic, land_sea):
    lon_count = lax.axis_size("lon")
    lat_count = lax.axis_size("lat")
    lat = lax.axis_index("lat")
    components, levels, band_rows, tile_cols = fields.shape
    total_rows = band_rows * lat_count
    pole_rows = cutoff.shape[0] // 2
    pole_bands = pole_rows // band_rows
    polar = (lat < pole_bands) | (lat >= lat_count - pole_bands)
    table, twist = fft_tables()
    table = jnp.asarray(table)
    table_hi, table_lo = split(table)
    twist = jnp.asarray(twist)
    at = jnp.where(lat < pole_bands, lat * band_rows, lat * band_rows - (total_rows - 2 * pole_rows))
    cuts = lax.dynamic_slice_in_dim(cutoff, jnp.clip(at, 0, 2 * pole_rows - band_rows), band_rows)
    per = components * levels // lon_count
    circles = per * band_rows
    cuts = jnp.tile(cuts, per)[None, :]
    flag = polar.astype(jnp.int32)[None]
    packed = (lon_count, tile_cols, circles)
    dma = pltpu.SemaphoreType.DMA((lon_count,))
    parts = pl.pallas_call(
        pack_kernel,
        out_shape=pltpu.HBM(packed, jnp.float32),
        in_specs=[sm(), hbm()],
        out_specs=hbm(),
        scratch_shapes=[
            pltpu.VMEM((components * levels, band_rows, tile_cols), jnp.float32),
            pltpu.VMEM(packed, jnp.float32),
            dma,
            dma,
        ],
        name="pack_circles",
        compiler_params=pltpu.CompilerParams(vmem_limit_bytes=60 * MIB),
    )(thickness, fields.reshape(components * levels, band_rows, tile_cols))
    parts = lax.all_to_all(parts, "lon", split_axis=0, concat_axis=0)
    east, west = barotropic_rims(barotropic, land_sea, shift)
    parts, east, west = lax.optimization_barrier((parts, east, west))
    parts = filter_call(flag, parts, cuts, table_hi, table_lo, twist)
    parts = lax.all_to_all(parts, "lon", split_axis=0, concat_axis=0)
    new, sea_level = barotropic_steps(barotropic, land_sea, east, west, lat, total_rows, shift)
    half = (components * levels // 2, band_rows, tile_cols)
    tracers, velocity = pl.pallas_call(
        unpack_kernel,
        out_shape=(pltpu.HBM(half, jnp.float32),) * 2,
        in_specs=[hbm(), vm()],
        out_specs=(hbm(), hbm()),
        scratch_shapes=[
            pltpu.VMEM(packed, jnp.float32),
            pltpu.VMEM((lon_count, per, band_rows, tile_cols), jnp.float32),
            dma,
            dma,
        ],
        name="unpack_circles",
        compiler_params=pltpu.CompilerParams(vmem_limit_bytes=20 * MIB),
    )(parts, new)
    shape = (2, levels, band_rows, tile_cols)
    return (tracers.reshape(shape), velocity.reshape(shape), sea_level)


def solution(mesh):
    return jax.shard_map(
        body,
        mesh=mesh,
        in_specs=(P(None, None, "lat", "lon"), P(), P(), P(None, "lat", "lon"), P("lat", "lon")),
        out_specs=(P(None, None, "lat", "lon"), P(None, None, "lat", "lon"), P("lat", "lon")),
        check_vma=False,
    )
```

```python
import math
import numpy as np
import jax
import jax.numpy as jnp
from jax import lax
from jax.experimental import pallas as pl
from jax.experimental.pallas import tpu as pltpu
from jax.sharding import PartitionSpec as P


WAVE = 0.65
SUB = 20
MIB = 1 << 20
RIM = 21
ROWH = 24
SEG = 225
HALF = SEG // 2
FOLD = 128
MROW = 120


def cplx_add(a, b):
    return (a[0] + b[0], (b[1] if a[1] is None else a[1] if b[1] is None else a[1] + b[1]))


def cplx_sub(a, b):
    if b[1] is None:
        im = a[1]
    elif a[1] is None:
        im = -b[1]
    else:
        im = a[1] - b[1]
    return (a[0] - b[0], im)


def conj(a):
    return (a[0], None if a[1] is None else -a[1])


def turn(a, num, den):
    num %= den
    if num == 0:
        return a
    c, s = math.cos(2 * math.pi * num / den), math.sin(2 * math.pi * num / den)
    re, im = a
    if (4 * num) % den == 0:
        q = 4 * num // den
        if q == 1:
            return (jnp.zeros_like(re) if im is None else -im, re)
        if q == 2:
            return (-re, None if im is None else -im)
        return (jnp.zeros_like(re) if im is None else im, -re)
    if im is None:
        return (re * c, re * s)
    if abs(abs(c) - abs(s)) < 1e-12:
        h = abs(c)
        sc, ss = math.copysign(1.0, c), math.copysign(1.0, s)
        x = re if sc > 0 else -re
        y = im if ss > 0 else -im
        x2 = re if ss > 0 else -re
        y2 = im if sc > 0 else -im
        return ((x - y) * h, (x2 + y2) * h)
    return (re * c - im * s, re * s + im * c)


def real_dft(xs):
    n = len(xs)
    if n == 2:
        return [(xs[0] + xs[1], None), (xs[0] - xs[1], None)]
    even, odd = real_dft(xs[0::2]), real_dft(xs[1::2])
    out = [None] * (n // 2 + 1)
    for r in range(n // 4 + 1):
        o = turn(odd[r], -r, n)
        out[r] = cplx_add(even[r], o)
        if r != n // 2 - r:
            out[n // 2 - r] = conj(cplx_sub(even[r], o))
    return out


def real_idft(ys):
    n = 2 * (len(ys) - 1)
    if n == 2:
        return [ys[0][0] + ys[1][0], ys[0][0] - ys[1][0]]
    even, odd = [], []
    for r in range(n // 4 + 1):
        a, b = ys[r], conj(ys[n // 2 - r])
        if r in (0,):
            a, b = (a[0], None), (b[0], None)
        if r == n // 4:
            even.append((a[0] + a[0], None))
            o = turn((a[0] - a[0], a[1] + a[1]), r, n) if False else None
            odd.append((-(a[1] + a[1]), None))
            continue
        even.append(cplx_add(a, b))
        odd.append(turn(cplx_sub(a, b), r, n))
    e, o = real_idft(even), real_idft(odd)
    out = [None] * n
    out[0::2], out[1::2] = e, o
    return out


def fft_tables():
    at = np.concatenate([np.arange(1, HALF + 1), [0]])
    ang = 2.0 * np.pi * ((at[:, None] * at[None, :]) % SEG) / SEG
    w = np.zeros((2, FOLD, 2 * FOLD), np.float32)
    for half in (0, FOLD):
        w[0, : HALF + 1, half : half + HALF + 1] = np.cos(ang) / 60.0
        w[1, : HALF + 1, half : half + HALF + 1] = np.sin(ang) / 60.0
    tw = np.zeros((HALF, 16), np.float32)
    for r in range(1, 9):
        a = 2.0 * np.pi * r * np.arange(1, HALF + 1) / (16 * SEG)
        tw[:, r - 1] = np.cos(a)
        tw[:, r + 7] = np.sin(a)
    return w, tw


def split(x):
    hi = x.astype(jnp.bfloat16)
    lo = (x - hi.astype(jnp.float32)).astype(jnp.bfloat16)
    return hi, lo


def backward(x):
    rows = 7 - lax.broadcasted_iota(jnp.int32, x.shape, 0)
    return jnp.take_along_axis(x, rows, axis=0)


def filter_kernel(
    polar_ref, x_hbm, cut_ref, wh_ref, wl_ref, tw_ref, y_hbm, x_ref, e_scr, o_scr, in_sem, out_sem
):
    polar = polar_ref[0] != 0
    lanes = x_ref.shape[2]
    groups = [pl.ds(128 * g, 128) for g in range(lanes // 128)]

    def get(g):
        at = (slice(None), slice(None), groups[g])
        return pltpu.make_async_copy(x_hbm.at[at], x_ref.at[at], in_sem.at[g])

    def put(g):
        at = (slice(None), slice(None), groups[g])
        return pltpu.make_async_copy(x_ref.at[at], y_hbm.at[at], out_sem.at[g])

    for g in range(lanes // 128):
        get(g).start()
    two = 2 * lanes

    @pl.when(jnp.logical_not(polar))
    def _():
        for g in range(lanes // 128):
            get(g).wait()
            put(g).start()

    @pl.when(polar)
    def _():
        e_scr[HALF:, :] = jnp.zeros((FOLD - HALF, 9 * two), jnp.float32)
        o_scr[HALF:, :] = jnp.zeros((FOLD - HALF, 9 * two), jnp.float32)

        def spots(g, r):
            at = r * two + g * 128
            return pl.ds(at, 128), pl.ds(at + lanes, 128)

        def twiddles(tw, r):
            c = jnp.broadcast_to(tw[:, r - 1 : r], (8, 128))
            s = jnp.broadcast_to(tw[:, r + 7 : r + 8], (8, 128))
            return c, s

        def forward(g):
            lane = groups[g]
            get(g).wait()
            first = real_dft([x_ref[s // 2, pl.ds(s % 2 * SEG, 1), lane] for s in range(16)])
            for r in range(9):
                re_at, im_at = spots(g, r)
                e_scr[HALF : HALF + 1, re_at] = first[r][0]
                if first[r][1] is not None:
                    e_scr[HALF : HALF + 1, im_at] = first[r][1]
            for i in range(HALF // 8):
                rows = pl.ds(8 * i, 8)
                tw = tw_ref[rows, :]
                za = real_dft([x_ref[s // 2, pl.ds(s % 2 * SEG + 8 * i + 1, 8), lane] for s in range(16)])
                far = [
                    backward(x_ref[s // 2, pl.ds(s % 2 * SEG + SEG - 8 - 8 * i, 8), lane])
                    for s in range(16)
                ]
                zb = real_dft(far[-1:] + far[:-1])
                re_at, im_at = spots(g, 0)
                e_scr[rows, re_at] = za[0][0] + zb[0][0]
                o_scr[rows, re_at] = za[0][0] - zb[0][0]
                for r in range(1, 9):
                    c, s = twiddles(tw, r)
                    (ar, ai), (br, bi) = za[r], zb[r]
                    if r == 8:
                        ure, uim, vre, vim = ar * c, -(ar * s), br * c, br * s
                    else:
                        ure, uim = ar * c + ai * s, ai * c - ar * s
                        vre, vim = br * c - bi * s, bi * c + br * s
                    re_at, im_at = spots(g, r)
                    e_scr[rows, re_at] = ure + vre
                    o_scr[rows, re_at] = ure - vre
                    e_scr[rows, im_at] = uim + vim
                    o_scr[rows, im_at] = uim - vim

        for g in range(lanes // 128):
            forward(g)
        row = lax.broadcasted_iota(jnp.int32, (MROW, lanes), 0)
        k16 = jnp.where(row < HALF, 16 * (row + 1), 0)
        cut = jnp.broadcast_to(cut_ref[...], (MROW, lanes))

        def product(which, x):
            both = jnp.concatenate(split(x), axis=0)
            f = lambda a: jnp.dot(a, both, preferred_element_type=jnp.float32)
            return (f(wh_ref[which]) + f(wl_ref[which]))[:MROW]

        for r in range(9):
            col = pl.ds(r * two, lanes if r == 0 else two)
            p, q = product(0, e_scr[:, col]), product(1, o_scr[:, col])
            pr, qr = p[:, :lanes], q[:, :lanes]
            near = k16 + r <= cut
            far = (k16 - r <= cut) & (row < HALF)
            if r == 0:
                ere = jnp.where(near, jnp.where(row < HALF, pr + pr, pr), 0.0)
                oim = jnp.where(near, -(qr + qr), 0.0)
                e_scr[0:MROW, col] = ere
                o_scr[0:MROW, col] = oim
                p, q = product(0, e_scr[:, col]), product(1, o_scr[:, col])
                e_scr[0:MROW, col] = p - q
                o_scr[0:MROW, col] = p + q
                continue
            pi, qi = p[:, lanes:], q[:, lanes:]
            xr = jnp.where(near, pr + qi, 0.0)
            xi = jnp.where(near, pi - qr, 0.0)
            yr = jnp.where(far, pr - qi, 0.0)
            yi = jnp.where(far, pi + qr, 0.0)
            e_scr[0:MROW, col] = jnp.concatenate([xr + yr, xi + yi], axis=1)
            o_scr[0:MROW, col] = jnp.concatenate([xr - yr, xi - yi], axis=1)
            p, q = product(0, e_scr[:, col]), product(1, o_scr[:, col])
            pr, qr, pi, qi = p[:, :lanes], q[:, :lanes], p[:, lanes:], q[:, lanes:]
            e_scr[0:MROW, col] = jnp.concatenate([pr - qi, pi + qr], axis=1)
            o_scr[0:MROW, col] = jnp.concatenate([pr + qi, pi - qr], axis=1)

        def inverse(g):
            lane = groups[g]
            ws = []
            for r in range(9):
                re_at, im_at = spots(g, r)
                im = None if r in (0, 8) else e_scr[HALF : HALF + 1, im_at]
                ws.append((e_scr[HALF : HALF + 1, re_at], im))
            ys = real_idft(ws)
            for s in range(16):
                x_ref[s // 2, pl.ds(s % 2 * SEG, 1), lane] = ys[s]
            for i in range(HALF // 8):
                rows = pl.ds(8 * i, 8)
                tw = tw_ref[rows, :]
                re_at, im_at = spots(g, 0)
                wa, wb = [(e_scr[rows, re_at], None)], [(o_scr[rows, re_at], None)]
                for r in range(1, 9):
                    re_at, im_at = spots(g, r)
                    c, s = twiddles(tw, r)
                    ar, ai, br, bi = e_scr[rows, re_at], e_scr[rows, im_at], o_scr[rows, re_at], o_scr[rows, im_at]
                    wa.append((ar * c - ai * s, None if r == 8 else ai * c + ar * s))
                    wb.append((br * c + bi * s, None if r == 8 else bi * c - br * s))
                ya, yb = real_idft(wa), real_idft(wb)
                for s in range(16):
                    x_ref[s // 2, pl.ds(s % 2 * SEG + 8 * i + 1, 8), lane] = ya[s]
                    x_ref[s // 2, pl.ds(s % 2 * SEG + SEG - 8 - 8 * i, 8), lane] = backward(yb[(s + 1) % 16])
            put(g).start()

        for g in range(lanes // 128):
            inverse(g)

    for g in range(lanes // 128):
        put(g).wait()


def filter_call(polar, x, cut, wh, wl, tw):
    lanes = x.shape[2]
    vmem = pl.BlockSpec(memory_space=pltpu.VMEM)
    far = pl.BlockSpec(memory_space=pltpu.HBM)
    dma = pltpu.SemaphoreType.DMA((lanes // 128,))
    return pl.pallas_call(
        filter_kernel,
        out_shape=pltpu.HBM(x.shape, jnp.float32),
        in_specs=[pl.BlockSpec(memory_space=pltpu.SMEM), far] + [vmem] * 4,
        out_specs=far,
        scratch_shapes=[
            pltpu.VMEM(x.shape, jnp.float32),
            pltpu.VMEM((FOLD, 9 * 2 * lanes), jnp.float32),
            pltpu.VMEM((FOLD, 9 * 2 * lanes), jnp.float32),
            dma,
            dma,
        ],
        name="polar_filter",
        compiler_params=pltpu.CompilerParams(vmem_limit_bytes=32 * MIB),
    )(polar, x, cut, wh, wl, tw)


ROWS = 64
COLS = 450
LANES = 512
FAR = 112


def lane_ids(rows):
    return lax.broadcasted_iota(jnp.int32, (rows, 128), 1)


def rim_kernel(flow_ref, land_ref, first_ref, last_ref, scr):
    lane = lane_ids(ROWS)
    first = jnp.zeros((ROWS, 128), jnp.float32)
    last = first
    for a in range(4):
        if a < 3:
            scr[:, 0:COLS] = flow_ref[a]
        else:
            scr[:, 0:COLS] = land_ref[...].astype(jnp.float32)
        mine = (lane >= RIM * a) & (lane < RIM * (a + 1))
        first = jnp.where(mine, pltpu.roll(scr[:, 0:128], RIM * a, 1), first)
        turn_by = (RIM * (a + 1) - (COLS - 384)) % 128
        last = jnp.where(mine, pltpu.roll(scr[:, 384:512], turn_by, 1), last)
    first_ref[...] = first
    last_ref[...] = last


def join_kernel(flow_ref, land_ref, east_ref, west_ref, mid_ref, top_ref, low_ref):
    lane = lane_ids(ROWS)
    for a in range(4):
        if a < 3:
            mid_ref[a, :, 0:COLS] = flow_ref[a]
        else:
            mid_ref[a, :, 0:COLS] = land_ref[...].astype(jnp.float32)
        own = mid_ref[a, :, 384:512]
        west = pltpu.roll(west_ref[...], 128 - RIM * (a + 1), 1)
        east = pltpu.roll(east_ref[...], (COLS - 384 - RIM * a) % 128, 1)
        west = jnp.where(lane >= 128 - RIM, west, 0.0)
        east = jnp.where(lane < COLS - 384 + RIM, east, west)
        mid_ref[a, :, 384:512] = jnp.where(lane < COLS - 384, own, east)
        top_ref[a] = mid_ref[a, 0:ROWH]
        low_ref[a] = mid_ref[a, ROWS - ROWH :]


def step_kernel(at_ref, mid_ref, top_ref, low_ref, out_ref, sea_ref, s_scr, e_scr, n_scr, oc_scr, eo_scr, no_scr):
    first_row = at_ref[0] * ROWS - ROWH
    total = at_ref[1]
    for a, scr in enumerate((s_scr, e_scr, n_scr, oc_scr)):
        scr[0:8] = jnp.zeros((8, LANES), jnp.float32)
        scr[8 + FAR :] = jnp.zeros((8, LANES), jnp.float32)
        scr[8 : 8 + ROWH] = top_ref[a]
        scr[8 + ROWH : 8 + ROWH + ROWS] = mid_ref[a]
        scr[8 + ROWH + ROWS : 8 + FAR] = low_ref[a]
    for b in range(FAR // 8):
        at = 8 + 8 * b
        oc = oc_scr[at : at + 8]
        row = first_row + 8 * b + lax.broadcasted_iota(jnp.int32, (8, LANES), 0)
        last = (row == total - 1) | (row == -1)
        eo = oc * pltpu.roll(oc, LANES - 1, 1)
        no = jnp.where(last, 0.0, oc * oc_scr[at + 1 : at + 9])
        eo_scr[at : at + 8] = eo
        no_scr[at : at + 8] = no
        e_scr[at : at + 8] = e_scr[at : at + 8] * eo
        n_scr[at : at + 8] = n_scr[at : at + 8] * no

    def step(_, carry):
        for b in range(FAR // 8):
            at = 8 + 8 * b
            e = e_scr[at : at + 8]
            div = e - pltpu.roll(e, 1, 1) + n_scr[at : at + 8] - n_scr[at - 1 : at + 7]
            s_scr[at : at + 8] = s_scr[at : at + 8] - WAVE * oc_scr[at : at + 8] * div
        for b in range(FAR // 8):
            at = 8 + 8 * b
            s = s_scr[at : at + 8]
            e_scr[at : at + 8] = eo_scr[at : at + 8] * (
                e_scr[at : at + 8] - WAVE * (pltpu.roll(s, LANES - 1, 1) - s)
            )
            n_scr[at : at + 8] = no_scr[at : at + 8] * (
                n_scr[at : at + 8] - WAVE * (s_scr[at + 1 : at + 9] - s)
            )
        return carry

    lax.fori_loop(0, SUB, step, 0)
    mine = slice(8 + ROWH, 8 + ROWH + ROWS)
    sea_ref[...] = s_scr[mine, 0:COLS]
    for a, scr in enumerate((e_scr, n_scr, eo_scr, no_scr)):
        out_ref[a] = scr[mine, 0:COLS]


def vm():
    return pl.BlockSpec(memory_space=pltpu.VMEM)


def hbm():
    return pl.BlockSpec(memory_space=pltpu.HBM)


def sm():
    return pl.BlockSpec(memory_space=pltpu.SMEM)


def f32(*dims):
    return jax.ShapeDtypeStruct(dims, jnp.float32)


def barotropic_rims(flow, land, shift):
    first, last = pl.pallas_call(
        rim_kernel,
        out_shape=(f32(ROWS, 128), f32(ROWS, 128)),
        in_specs=[vm(), vm()],
        out_specs=(vm(), vm()),
        scratch_shapes=[pltpu.VMEM((ROWS, LANES), jnp.float32)],
        name="rim_columns",
        compiler_params=pltpu.CompilerParams(vmem_limit_bytes=8 * MIB),
    )(flow, land)
    east = shift(first, "lon", -1)
    west = shift(last, "lon", 1)
    return east, west


def barotropic_steps(flow, land, east, west, lat_index, total_rows, shift):
    mid, top, low = pl.pallas_call(
        join_kernel,
        out_shape=(f32(4, ROWS, LANES), f32(4, ROWH, LANES), f32(4, ROWH, LANES)),
        in_specs=[vm()] * 4,
        out_specs=(vm(), vm(), vm()),
        name="join_columns",
        compiler_params=pltpu.CompilerParams(vmem_limit_bytes=8 * MIB),
    )(flow, land, east, west)
    above = shift(low, "lat", 1)
    below = shift(top, "lat", -1)
    where = jnp.stack([lat_index, jnp.int32(total_rows)])
    return pl.pallas_call(
        step_kernel,
        out_shape=(f32(4, ROWS, COLS), f32(ROWS, COLS)),
        in_specs=[sm()] + [vm()] * 3,
        out_specs=(vm(), vm()),
        scratch_shapes=[pltpu.VMEM((FAR + 16, LANES), jnp.float32)] * 6,
        name="subcycles",
        compiler_params=pltpu.CompilerParams(vmem_limit_bytes=8 * MIB),
    )(where, mid, above, below)


def pack_kernel(thick_ref, x_hbm, out_hbm, x_scr, y_scr, in_sem, out_sem):
    parts = out_hbm.shape[0]
    per = x_hbm.shape[0] // parts
    levels = thick_ref.shape[0]
    tracer_parts = parts // 2
    gets = []
    for p in range(parts):
        span = pl.ds(p * per, per)
        gets.append(pltpu.make_async_copy(x_hbm.at[span], x_scr.at[span], in_sem.at[p]))
        gets[-1].start()
    puts = []

    def put(p, xs):
        y_scr[p] = jnp.concatenate(xs, axis=0).T
        puts.append(pltpu.make_async_copy(y_scr.at[p], out_hbm.at[p], out_sem.at[p]))
        puts[-1].start()

    for p in range(tracer_parts):
        gets[p].wait()
        put(p, [x_scr[p * per + i] for i in range(per)])
    whole = thick_ref[0]
    for k in range(1, levels):
        whole = whole + thick_ref[k]
    scale = 1.0 / jnp.full((1, COLS), whole, jnp.float32)
    group = levels // per
    for p in range(tracer_parts, parts, group):
        for q in range(group):
            gets[p + q].wait()
        mean = thick_ref[0] * x_scr[p * per]
        for k in range(1, levels):
            mean = mean + thick_ref[k] * x_scr[p * per + k]
        mean = mean * scale
        for q in range(group):
            put(p + q, [x_scr[(p + q) * per + i] - mean for i in range(per)])
    for copy in puts:
        copy.wait()


def unpack_kernel(got_hbm, new_ref, tracer_hbm, speed_hbm, x_scr, y_scr, in_sem, out_sem):
    parts = got_hbm.shape[0]
    held = parts // 2
    per = tracer_hbm.shape[0] // held
    gets, puts = [], []
    for p in range(parts):
        gets.append(pltpu.make_async_copy(got_hbm.at[p], x_scr.at[p], in_sem.at[p]))
        gets[-1].start()
    for p in range(parts):
        gets[p].wait()
        block = x_scr[p].T
        for k in range(per):
            piece = block[k * ROWS : (k + 1) * ROWS]
            if p >= held:
                field = (p - held) // (held // 2)
                piece = new_ref[2 + field] * (piece + new_ref[field])
            y_scr[p, k] = piece
        to = tracer_hbm if p < held else speed_hbm
        span = pl.ds(p % held * per, per)
        puts.append(pltpu.make_async_copy(y_scr.at[p], to.at[span], out_sem.at[p]))
        puts[-1].start()
    for copy in puts:
        copy.wait()


def shift(value, axis, by):
    size = lax.axis_size(axis)
    return lax.ppermute(value, axis, [(i, (i + by) % size) for i in range(size)])


def body(fields, thickness, cutoff, barotropic, land_sea):
    lon_count = lax.axis_size("lon")
    lat_count = lax.axis_size("lat")
    lat = lax.axis_index("lat")
    components, levels, band_rows, tile_cols = fields.shape
    total_rows = band_rows * lat_count
    pole_rows = cutoff.shape[0] // 2
    pole_bands = pole_rows // band_rows
    polar = (lat < pole_bands) | (lat >= lat_count - pole_bands)
    table, twist = fft_tables()
    table = jnp.asarray(table)
    table_hi, table_lo = split(table)
    twist = jnp.asarray(twist)
    at = jnp.where(lat < pole_bands, lat * band_rows, lat * band_rows - (total_rows - 2 * pole_rows))
    cuts = lax.dynamic_slice_in_dim(cutoff, jnp.clip(at, 0, 2 * pole_rows - band_rows), band_rows)
    per = components * levels // lon_count
    circles = per * band_rows
    cuts = jnp.tile(cuts, per)[None, :]
    flag = polar.astype(jnp.int32)[None]
    packed = (lon_count, tile_cols, circles)
    dma = pltpu.SemaphoreType.DMA((lon_count,))
    parts = pl.pallas_call(
        pack_kernel,
        out_shape=pltpu.HBM(packed, jnp.float32),
        in_specs=[sm(), hbm()],
        out_specs=hbm(),
        scratch_shapes=[
            pltpu.VMEM((components * levels, band_rows, tile_cols), jnp.float32),
            pltpu.VMEM(packed, jnp.float32),
            dma,
            dma,
        ],
        name="pack_circles",
        compiler_params=pltpu.CompilerParams(vmem_limit_bytes=60 * MIB),
    )(thickness, fields.reshape(components * levels, band_rows, tile_cols))
    parts = lax.all_to_all(parts, "lon", split_axis=0, concat_axis=0)
    east, west = barotropic_rims(barotropic, land_sea, shift)
    parts = filter_call(flag, parts, cuts, table_hi, table_lo, twist)
    parts = lax.all_to_all(parts, "lon", split_axis=0, concat_axis=0)
    new, sea_level = barotropic_steps(barotropic, land_sea, east, west, lat, total_rows, shift)
    half = (components * levels // 2, band_rows, tile_cols)
    tracers, velocity = pl.pallas_call(
        unpack_kernel,
        out_shape=(pltpu.HBM(half, jnp.float32),) * 2,
        in_specs=[hbm(), vm()],
        out_specs=(hbm(), hbm()),
        scratch_shapes=[
            pltpu.VMEM(packed, jnp.float32),
            pltpu.VMEM((lon_count, per, band_rows, tile_cols), jnp.float32),
            dma,
            dma,
        ],
        name="unpack_circles",
        compiler_params=pltpu.CompilerParams(vmem_limit_bytes=20 * MIB),
    )(parts, new)
    shape = (2, levels, band_rows, tile_cols)
    return (tracers.reshape(shape), velocity.reshape(shape), sea_level)


def solution(mesh):
    return jax.shard_map(
        body,
        mesh=mesh,
        in_specs=(P(None, None, "lat", "lon"), P(), P(), P(None, "lat", "lon"), P("lat", "lon")),
        out_specs=(P(None, None, "lat", "lon"), P(None, None, "lat", "lon"), P("lat", "lon")),
        check_vma=False,
    )
```

```python
import functools
import math
import numpy as np
import jax
import jax.numpy as jnp
from jax import lax
from jax.experimental import pallas as pl
from jax.experimental.pallas import tpu as pltpu
from jax.sharding import PartitionSpec as P


WAVE = 0.65
SUB = 20
POLE_ROWS = 128
MIB = 1 << 20
RIM = 21
ROWH = 24
SEG = 225
HALF = SEG // 2
FOLD = 128
MROW = 120


def cplx_add(a, b):
    return (a[0] + b[0], (b[1] if a[1] is None else a[1] if b[1] is None else a[1] + b[1]))


def cplx_sub(a, b):
    if b[1] is None:
        im = a[1]
    elif a[1] is None:
        im = -b[1]
    else:
        im = a[1] - b[1]
    return (a[0] - b[0], im)


def conj(a):
    return (a[0], None if a[1] is None else -a[1])


def turn(a, num, den):
    num %= den
    if num == 0:
        return a
    c, s = math.cos(2 * math.pi * num / den), math.sin(2 * math.pi * num / den)
    re, im = a
    if (4 * num) % den == 0:
        q = 4 * num // den
        if q == 1:
            return (jnp.zeros_like(re) if im is None else -im, re)
        if q == 2:
            return (-re, None if im is None else -im)
        return (jnp.zeros_like(re) if im is None else im, -re)
    if im is None:
        return (re * c, re * s)
    if abs(abs(c) - abs(s)) < 1e-12:
        h = abs(c)
        sc, ss = math.copysign(1.0, c), math.copysign(1.0, s)
        x = re if sc > 0 else -re
        y = im if ss > 0 else -im
        x2 = re if ss > 0 else -re
        y2 = im if sc > 0 else -im
        return ((x - y) * h, (x2 + y2) * h)
    return (re * c - im * s, re * s + im * c)


def real_dft(xs):
    n = len(xs)
    if n == 2:
        return [(xs[0] + xs[1], None), (xs[0] - xs[1], None)]
    even, odd = real_dft(xs[0::2]), real_dft(xs[1::2])
    out = [None] * (n // 2 + 1)
    for r in range(n // 4 + 1):
        o = turn(odd[r], -r, n)
        out[r] = cplx_add(even[r], o)
        if r != n // 2 - r:
            out[n // 2 - r] = conj(cplx_sub(even[r], o))
    return out


def real_idft(ys):
    n = 2 * (len(ys) - 1)
    if n == 2:
        return [ys[0][0] + ys[1][0], ys[0][0] - ys[1][0]]
    even, odd = [], []
    for r in range(n // 4 + 1):
        a, b = ys[r], conj(ys[n // 2 - r])
        if r in (0,):
            a, b = (a[0], None), (b[0], None)
        if r == n // 4:
            even.append((a[0] + a[0], None))
            o = turn((a[0] - a[0], a[1] + a[1]), r, n) if False else None
            odd.append((-(a[1] + a[1]), None))
            continue
        even.append(cplx_add(a, b))
        odd.append(turn(cplx_sub(a, b), r, n))
    e, o = real_idft(even), real_idft(odd)
    out = [None] * n
    out[0::2], out[1::2] = e, o
    return out


def fft_tables():
    at = np.concatenate([np.arange(1, HALF + 1), [0]])
    ang = 2.0 * np.pi * ((at[:, None] * at[None, :]) % SEG) / SEG
    w = np.zeros((2, FOLD, 2 * FOLD), np.float32)
    for half in (0, FOLD):
        w[0, : HALF + 1, half : half + HALF + 1] = np.cos(ang) / 60.0
        w[1, : HALF + 1, half : half + HALF + 1] = np.sin(ang) / 60.0
    tw = np.zeros((HALF, 16), np.float32)
    for r in range(1, 9):
        a = 2.0 * np.pi * r * np.arange(1, HALF + 1) / (16 * SEG)
        tw[:, r - 1] = np.cos(a)
        tw[:, r + 7] = np.sin(a)
    return w, tw


def split(x):
    hi = x.astype(jnp.bfloat16)
    lo = (x - hi.astype(jnp.float32)).astype(jnp.bfloat16)
    return hi, lo


def backward(x):
    rows = 7 - lax.broadcasted_iota(jnp.int32, x.shape, 0)
    return jnp.take_along_axis(x, rows, axis=0)


def whereabouts():
    lat, bands = lax.axis_index("lat"), lax.axis_size("lat")
    edge = POLE_ROWS // ROWS
    return (lat < edge) | (lat >= bands - edge), lax.axis_index("lon")


def filter_kernel(*refs, slots):
    xs = refs[:slots]
    cut_ref, wh_ref, wl_ref, tw_ref = refs[slots : 4 + slots]
    y_hbm, y_ref, e_scr, o_scr, out_sem = refs[-5:]
    polar, lon = whereabouts()
    seats, _, lanes = y_ref.shape
    groups = [pl.ds(0, lanes)]

    def load(d, rows):
        return xs[0][d, rows, :] if slots == 1 else xs[d][rows, :]

    def put(d, where=y_ref):
        to = d if slots == 1 else (lon + d) % seats
        return pltpu.make_async_copy(where.at[d], y_hbm.at[to], out_sem.at[d])

    two = 2 * lanes

    if slots == 1:

        @pl.when(jnp.logical_not(polar))
        def _():
            for d in range(seats):
                put(d, xs[0]).start()
            for d in range(seats):
                put(d, xs[0]).wait()

    @pl.when(polar)
    def _():
        e_scr[HALF:, :] = jnp.zeros((FOLD - HALF, 9 * two), jnp.float32)
        o_scr[HALF:, :] = jnp.zeros((FOLD - HALF, 9 * two), jnp.float32)

        def spots(g, r):
            at = r * two + g * 128
            return pl.ds(at, 128), pl.ds(at + lanes, 128)

        def twiddles(tw, r):
            c = jnp.broadcast_to(tw[:, r - 1 : r], (8, 128))
            s = jnp.broadcast_to(tw[:, r + 7 : r + 8], (8, 128))
            return c, s

        def forward(g):
            first = real_dft([load(s // 2, pl.ds(s % 2 * SEG, 1)) for s in range(16)])
            for r in range(9):
                re_at, im_at = spots(g, r)
                e_scr[HALF : HALF + 1, re_at] = first[r][0]
                if first[r][1] is not None:
                    e_scr[HALF : HALF + 1, im_at] = first[r][1]
            for i in range(HALF // 8):
                rows = pl.ds(8 * i, 8)
                tw = tw_ref[rows, :]
                za = real_dft([load(s // 2, pl.ds(s % 2 * SEG + 8 * i + 1, 8)) for s in range(16)])
                far = [
                    backward(load(s // 2, pl.ds(s % 2 * SEG + SEG - 8 - 8 * i, 8)))
                    for s in range(16)
                ]
                zb = real_dft(far[-1:] + far[:-1])
                re_at, im_at = spots(g, 0)
                e_scr[rows, re_at] = za[0][0] + zb[0][0]
                o_scr[rows, re_at] = za[0][0] - zb[0][0]
                for r in range(1, 9):
                    c, s = twiddles(tw, r)
                    (ar, ai), (br, bi) = za[r], zb[r]
                    if r == 8:
                        ure, uim, vre, vim = ar * c, -(ar * s), br * c, br * s
                    else:
                        ure, uim = ar * c + ai * s, ai * c - ar * s
                        vre, vim = br * c - bi * s, bi * c + br * s
                    re_at, im_at = spots(g, r)
                    e_scr[rows, re_at] = ure + vre
                    o_scr[rows, re_at] = ure - vre
                    e_scr[rows, im_at] = uim + vim
                    o_scr[rows, im_at] = uim - vim

        for g in range(lanes // 128):
            forward(g)
        row = lax.broadcasted_iota(jnp.int32, (MROW, lanes), 0)
        k16 = jnp.where(row < HALF, 16 * (row + 1), 0)
        cut = jnp.broadcast_to(cut_ref[...], (MROW, lanes))

        def product(which, x):
            both = jnp.concatenate(split(x), axis=0)
            f = lambda a: jnp.dot(a, both, preferred_element_type=jnp.float32)
            return (f(wh_ref[which]) + f(wl_ref[which]))[:MROW]

        for r in range(9):
            col = pl.ds(r * two, lanes if r == 0 else two)
            p, q = product(0, e_scr[:, col]), product(1, o_scr[:, col])
            pr, qr = p[:, :lanes], q[:, :lanes]
            near = k16 + r <= cut
            far = (k16 - r <= cut) & (row < HALF)
            if r == 0:
                ere = jnp.where(near, jnp.where(row < HALF, pr + pr, pr), 0.0)
                oim = jnp.where(near, -(qr + qr), 0.0)
                e_scr[0:MROW, col] = ere
                o_scr[0:MROW, col] = oim
                p, q = product(0, e_scr[:, col]), product(1, o_scr[:, col])
                e_scr[0:MROW, col] = p - q
                o_scr[0:MROW, col] = p + q
                continue
            pi, qi = p[:, lanes:], q[:, lanes:]
            xr = jnp.where(near, pr + qi, 0.0)
            xi = jnp.where(near, pi - qr, 0.0)
            yr = jnp.where(far, pr - qi, 0.0)
            yi = jnp.where(far, pi + qr, 0.0)
            e_scr[0:MROW, col] = jnp.concatenate([xr + yr, xi + yi], axis=1)
            o_scr[0:MROW, col] = jnp.concatenate([xr - yr, xi - yi], axis=1)
            p, q = product(0, e_scr[:, col]), product(1, o_scr[:, col])
            pr, qr, pi, qi = p[:, :lanes], q[:, :lanes], p[:, lanes:], q[:, lanes:]
            e_scr[0:MROW, col] = jnp.concatenate([pr - qi, pi + qr], axis=1)
            o_scr[0:MROW, col] = jnp.concatenate([pr + qi, pi - qr], axis=1)

        def inverse(g):
            lane = groups[g]
            ws = []
            for r in range(9):
                re_at, im_at = spots(g, r)
                im = None if r in (0, 8) else e_scr[HALF : HALF + 1, im_at]
                ws.append((e_scr[HALF : HALF + 1, re_at], im))
            ys = real_idft(ws)
            for s in range(16):
                y_ref[s // 2, pl.ds(s % 2 * SEG, 1), lane] = ys[s]
            for i in range(HALF // 8):
                rows = pl.ds(8 * i, 8)
                tw = tw_ref[rows, :]
                re_at, im_at = spots(g, 0)
                wa, wb = [(e_scr[rows, re_at], None)], [(o_scr[rows, re_at], None)]
                for r in range(1, 9):
                    re_at, im_at = spots(g, r)
                    c, s = twiddles(tw, r)
                    ar, ai, br, bi = e_scr[rows, re_at], e_scr[rows, im_at], o_scr[rows, re_at], o_scr[rows, im_at]
                    wa.append((ar * c - ai * s, None if r == 8 else ai * c + ar * s))
                    wb.append((br * c + bi * s, None if r == 8 else bi * c - br * s))
                ya, yb = real_idft(wa), real_idft(wb)
                for s in range(16):
                    y_ref[s // 2, pl.ds(s % 2 * SEG + 8 * i + 1, 8), lane] = ya[s]
                    y_ref[s // 2, pl.ds(s % 2 * SEG + SEG - 8 - 8 * i, 8), lane] = backward(yb[(s + 1) % 16])

        for g in range(lanes // 128):
            inverse(g)
        for d in range(seats):
            put(d).start()
        for d in range(seats):
            put(d).wait()


def filter_call(xs, cut, tables, twist, shape):
    lanes = xs[0].shape[-1]
    seats = shape[0]
    vmem = pl.BlockSpec(memory_space=pltpu.VMEM)
    far = pl.BlockSpec(memory_space=pltpu.HBM)
    dma = pltpu.SemaphoreType.DMA((seats,))
    operands = (*xs, cut, *tables, twist)
    return pl.pallas_call(
        functools.partial(filter_kernel, slots=len(xs)),
        out_shape=pltpu.HBM(shape, jnp.float32),
        in_specs=[vmem] * len(operands),
        out_specs=far,
        scratch_shapes=[
            pltpu.VMEM((seats, 2 * SEG, lanes), jnp.float32),
            pltpu.VMEM((FOLD, 9 * 2 * lanes), jnp.float32),
            pltpu.VMEM((FOLD, 9 * 2 * lanes), jnp.float32),
            dma,
        ],
        name="polar_filter",
        compiler_params=pltpu.CompilerParams(vmem_limit_bytes=20 * MIB),
    )(*operands)


ROWS = 64
COLS = 450
LANES = 512
FAR = 112


def lane_ids(rows):
    return lax.broadcasted_iota(jnp.int32, (rows, 128), 1)


def rim_kernel(flow_ref, land_ref, first_ref, last_ref, scr):
    lane = lane_ids(ROWS)
    first = jnp.zeros((ROWS, 128), jnp.float32)
    last = first
    for a in range(4):
        if a < 3:
            scr[:, 0:COLS] = flow_ref[a]
        else:
            scr[:, 0:COLS] = land_ref[...].astype(jnp.float32)
        mine = (lane >= RIM * a) & (lane < RIM * (a + 1))
        first = jnp.where(mine, pltpu.roll(scr[:, 0:128], RIM * a, 1), first)
        turn_by = (RIM * (a + 1) - (COLS - 384)) % 128
        last = jnp.where(mine, pltpu.roll(scr[:, 384:512], turn_by, 1), last)
    first_ref[...] = first
    last_ref[...] = last


def join_kernel(flow_ref, land_ref, east_ref, west_ref, mid_ref, top_ref, low_ref):
    lane = lane_ids(ROWS)
    for a in range(4):
        if a < 3:
            mid_ref[a, :, 0:COLS] = flow_ref[a]
        else:
            mid_ref[a, :, 0:COLS] = land_ref[...].astype(jnp.float32)
        own = mid_ref[a, :, 384:512]
        west = pltpu.roll(west_ref[...], 128 - RIM * (a + 1), 1)
        east = pltpu.roll(east_ref[...], (COLS - 384 - RIM * a) % 128, 1)
        west = jnp.where(lane >= 128 - RIM, west, 0.0)
        east = jnp.where(lane < COLS - 384 + RIM, east, west)
        mid_ref[a, :, 384:512] = jnp.where(lane < COLS - 384, own, east)
        top_ref[a] = mid_ref[a, 0:ROWH]
        low_ref[a] = mid_ref[a, ROWS - ROWH :]


def step_kernel(at_ref, mid_ref, top_ref, low_ref, out_ref, sea_ref, s_scr, e_scr, n_scr, oc_scr, eo_scr, no_scr):
    first_row = at_ref[0] * ROWS - ROWH
    total = at_ref[1]
    for a, scr in enumerate((s_scr, e_scr, n_scr, oc_scr)):
        scr[0:8] = jnp.zeros((8, LANES), jnp.float32)
        scr[8 + FAR :] = jnp.zeros((8, LANES), jnp.float32)
        scr[8 : 8 + ROWH] = top_ref[a]
        scr[8 + ROWH : 8 + ROWH + ROWS] = mid_ref[a]
        scr[8 + ROWH + ROWS : 8 + FAR] = low_ref[a]
    for b in range(FAR // 8):
        at = 8 + 8 * b
        oc = oc_scr[at : at + 8]
        row = first_row + 8 * b + lax.broadcasted_iota(jnp.int32, (8, LANES), 0)
        last = (row == total - 1) | (row == -1)
        eo = oc * pltpu.roll(oc, LANES - 1, 1)
        no = jnp.where(last, 0.0, oc * oc_scr[at + 1 : at + 9])
        eo_scr[at : at + 8] = eo
        no_scr[at : at + 8] = no
        e_scr[at : at + 8] = e_scr[at : at + 8] * eo
        n_scr[at : at + 8] = n_scr[at : at + 8] * no

    def step(_, carry):
        for b in range(FAR // 8):
            at = 8 + 8 * b
            e = e_scr[at : at + 8]
            div = e - pltpu.roll(e, 1, 1) + n_scr[at : at + 8] - n_scr[at - 1 : at + 7]
            s_scr[at : at + 8] = s_scr[at : at + 8] - WAVE * oc_scr[at : at + 8] * div
        for b in range(FAR // 8):
            at = 8 + 8 * b
            s = s_scr[at : at + 8]
            e_scr[at : at + 8] = eo_scr[at : at + 8] * (
                e_scr[at : at + 8] - WAVE * (pltpu.roll(s, LANES - 1, 1) - s)
            )
            n_scr[at : at + 8] = no_scr[at : at + 8] * (
                n_scr[at : at + 8] - WAVE * (s_scr[at + 1 : at + 9] - s)
            )
        return carry

    lax.fori_loop(0, SUB, step, 0)
    mine = slice(8 + ROWH, 8 + ROWH + ROWS)
    sea_ref[...] = s_scr[mine, 0:COLS]
    for a, scr in enumerate((e_scr, n_scr, eo_scr, no_scr)):
        out_ref[a] = scr[mine, 0:COLS]


def vm():
    return pl.BlockSpec(memory_space=pltpu.VMEM)


def hbm():
    return pl.BlockSpec(memory_space=pltpu.HBM)


def sm():
    return pl.BlockSpec(memory_space=pltpu.SMEM)


def f32(*dims):
    return jax.ShapeDtypeStruct(dims, jnp.float32)


def barotropic_rims(flow, land, shift):
    first, last = pl.pallas_call(
        rim_kernel,
        out_shape=(f32(ROWS, 128), f32(ROWS, 128)),
        in_specs=[vm(), vm()],
        out_specs=(vm(), vm()),
        scratch_shapes=[pltpu.VMEM((ROWS, LANES), jnp.float32)],
        name="rim_columns",
        compiler_params=pltpu.CompilerParams(vmem_limit_bytes=8 * MIB),
    )(flow, land)
    east = shift(first, "lon", -1)
    west = shift(last, "lon", 1)
    return east, west


def barotropic_steps(flow, land, east, west, lat_index, total_rows, shift):
    mid, top, low = pl.pallas_call(
        join_kernel,
        out_shape=(f32(4, ROWS, LANES), f32(4, ROWH, LANES), f32(4, ROWH, LANES)),
        in_specs=[vm()] * 4,
        out_specs=(vm(), vm(), vm()),
        name="join_columns",
        compiler_params=pltpu.CompilerParams(vmem_limit_bytes=8 * MIB),
    )(flow, land, east, west)
    above = shift(low, "lat", 1)
    below = shift(top, "lat", -1)
    where = jnp.stack([lat_index, jnp.int32(total_rows)])
    return pl.pallas_call(
        step_kernel,
        out_shape=(f32(4, ROWS, COLS), f32(ROWS, COLS)),
        in_specs=[sm()] + [vm()] * 3,
        out_specs=(vm(), vm()),
        scratch_shapes=[pltpu.VMEM((FAR + 16, LANES), jnp.float32)] * 6,
        name="subcycles",
        compiler_params=pltpu.CompilerParams(vmem_limit_bytes=8 * MIB),
    )(where, mid, above, below)


def pack_flow_kernel(thick_ref, x_hbm, out_hbm, x_scr, y_scr, in_sem, out_sem):
    parts = out_hbm.shape[0]
    levels = thick_ref.shape[0]
    skip = x_hbm.shape[0] // 2
    per = skip // parts
    gets, puts = [], []
    for p in range(parts):
        span = pl.ds(skip + p * per, per)
        gets.append(pltpu.make_async_copy(x_hbm.at[span], x_scr.at[pl.ds(p * per, per)], in_sem.at[p]))
        gets[-1].start()
    whole = thick_ref[0]
    for k in range(1, levels):
        whole = whole + thick_ref[k]
    scale = 1.0 / jnp.full((1, COLS), whole, jnp.float32)
    group = levels // per
    for p in range(0, parts, group):
        for q in range(group):
            gets[p + q].wait()
        mean = thick_ref[0] * x_scr[p * per]
        for k in range(1, levels):
            mean = mean + thick_ref[k] * x_scr[p * per + k]
        mean = mean * scale
        for q in range(p, p + group):
            y_scr[q] = jnp.concatenate([x_scr[q * per + i] - mean for i in range(per)], axis=0).T
            puts.append(pltpu.make_async_copy(y_scr.at[q], out_hbm.at[q], out_sem.at[q]))
            puts[-1].start()
    for copy in puts:
        copy.wait()


def pack_tracer_kernel(x_hbm, *refs):
    parts = len(refs) - 4
    outs = refs[:parts]
    x_scr, y_scr, in_sem, out_sem = refs[parts:]
    per = x_scr.shape[1]
    polar, lon = whereabouts()

    @pl.when(polar)
    def _():
        gets, puts = [], []
        for k in range(parts):
            span = pl.ds((lon + parts - k) % parts * per, per)
            gets.append(pltpu.make_async_copy(x_hbm.at[span], x_scr.at[k], in_sem.at[k]))
            gets[-1].start()
        for k in range(parts):
            gets[k].wait()
            y_scr[k] = jnp.concatenate([x_scr[k, i] for i in range(per)], axis=0).T
            puts.append(pltpu.make_async_copy(y_scr.at[k], outs[k], out_sem.at[k]))
            puts[-1].start()
        for copy in puts:
            copy.wait()


def unpack_flow_kernel(got_ref, new_ref, speed_hbm, v_scr, v_sem):
    parts = got_ref.shape[0]
    per = speed_hbm.shape[0] // parts
    puts = []
    for p in range(parts):
        field = p // (parts // 2)
        block = got_ref[p].T
        for k in range(per):
            piece = block[k * ROWS : (k + 1) * ROWS]
            v_scr[p, k] = new_ref[2 + field] * (piece + new_ref[field])
        puts.append(pltpu.make_async_copy(v_scr.at[p], speed_hbm.at[pl.ds(p * per, per)], v_sem.at[p]))
        puts[-1].start()
    for copy in puts:
        copy.wait()


def unpack_tracer_kernel(got_hbm, x_hbm, tracer_hbm, got_scr, t_scr, in_sem, out_sem):
    parts = got_hbm.shape[0]
    per = tracer_hbm.shape[0] // parts
    polar, _ = whereabouts()

    def get(p):
        return pltpu.make_async_copy(got_hbm.at[p], got_scr.at[p], in_sem.at[p])

    def keep(p):
        return pltpu.make_async_copy(x_hbm.at[pl.ds(p * per, per)], t_scr.at[p], in_sem.at[p])

    def put(p):
        return pltpu.make_async_copy(t_scr.at[p], tracer_hbm.at[pl.ds(p * per, per)], out_sem.at[p])

    @pl.when(polar)
    def _():
        for p in range(parts):
            get(p).start()
        for p in range(parts):
            get(p).wait()
            block = got_scr[p].T
            for k in range(per):
                t_scr[p, k] = block[k * ROWS : (k + 1) * ROWS]
            put(p).start()

    @pl.when(jnp.logical_not(polar))
    def _():
        for p in range(parts):
            keep(p).start()
        for p in range(parts):
            keep(p).wait()
            put(p).start()

    for p in range(parts):
        put(p).wait()


def shift(value, axis, by):
    size = lax.axis_size(axis)
    return lax.ppermute(value, axis, [(i, (i + by) % size) for i in range(size)])


def body(fields, thickness, cutoff, barotropic, land_sea):
    lon_count = lax.axis_size("lon")
    lat_count = lax.axis_size("lat")
    lat = lax.axis_index("lat")
    components, levels, band_rows, tile_cols = fields.shape
    total_rows = band_rows * lat_count
    pole_rows = cutoff.shape[0] // 2
    pole_bands = pole_rows // band_rows
    bands = [b for b in range(lat_count) if b < pole_bands or b >= lat_count - pole_bands]
    table, twist = fft_tables()
    tables = split(jnp.asarray(table))
    twist = jnp.asarray(twist)
    at = jnp.where(lat < pole_bands, lat * band_rows, lat * band_rows - (total_rows - 2 * pole_rows))
    cuts = lax.dynamic_slice_in_dim(cutoff, jnp.clip(at, 0, 2 * pole_rows - band_rows), band_rows)
    pairs = components * levels
    per = pairs // 2 // lon_count
    half = per * band_rows
    cuts = jnp.tile(cuts, per)[None, :]
    dma = pltpu.SemaphoreType.DMA((lon_count,))
    seats = range(lon_count)
    rows_in = fields.reshape(pairs, band_rows, tile_cols)
    parts = pl.pallas_call(
        pack_flow_kernel,
        out_shape=pltpu.HBM((lon_count, tile_cols, half), jnp.float32),
        in_specs=[sm(), hbm()],
        out_specs=hbm(),
        scratch_shapes=[
            pltpu.VMEM((pairs // 2, band_rows, tile_cols), jnp.float32),
            pltpu.VMEM((lon_count, tile_cols, half), jnp.float32),
            dma,
            dma,
        ],
        name="pack_flow",
        compiler_params=pltpu.CompilerParams(vmem_limit_bytes=60 * MIB),
    )(thickness, rows_in)
    parts = lax.all_to_all(parts, "lon", split_axis=0, concat_axis=0)
    slots = pl.pallas_call(
        pack_tracer_kernel,
        out_shape=[pltpu.HBM((tile_cols, half), jnp.float32) for _ in seats],
        in_specs=[hbm()],
        out_specs=[hbm() for _ in seats],
        scratch_shapes=[
            pltpu.VMEM((lon_count, per, band_rows, tile_cols), jnp.float32),
            pltpu.VMEM((lon_count, tile_cols, half), jnp.float32),
            dma,
            dma,
        ],
        name="pack_tracers",
        compiler_params=pltpu.CompilerParams(vmem_limit_bytes=60 * MIB),
    )(rows_in)
    got = [slots[0]]
    for k in range(1, lon_count):
        route = [
            (i * lat_count + b, (i + lon_count - k) % lon_count * lat_count + b) for b in bands for i in seats
        ]
        got.append(lax.ppermute(slots[k], ("lon", "lat"), route))
    shape = (lon_count, tile_cols, half)
    parts = filter_call([parts], cuts, tables, twist, shape)
    parts = lax.all_to_all(parts, "lon", split_axis=0, concat_axis=0)
    east, west = barotropic_rims(barotropic, land_sea, shift)
    got = filter_call(got, cuts, tables, twist, shape)
    got = lax.all_to_all(got, "lon", split_axis=0, concat_axis=0)
    new, sea_level = barotropic_steps(barotropic, land_sea, east, west, lat, total_rows, shift)
    out = pltpu.HBM((pairs // 2, band_rows, tile_cols), jnp.float32)
    rows_scr = pltpu.VMEM((lon_count, per, band_rows, tile_cols), jnp.float32)
    velocity = pl.pallas_call(
        unpack_flow_kernel,
        out_shape=out,
        in_specs=[vm(), vm()],
        out_specs=hbm(),
        scratch_shapes=[rows_scr, dma],
        name="unpack_flow",
        compiler_params=pltpu.CompilerParams(vmem_limit_bytes=16 * MIB),
    )(parts, new)
    tracers = pl.pallas_call(
        unpack_tracer_kernel,
        out_shape=out,
        in_specs=[hbm(), hbm()],
        out_specs=hbm(),
        scratch_shapes=[pltpu.VMEM(shape, jnp.float32), rows_scr, dma, dma],
        name="unpack_tracers",
        compiler_params=pltpu.CompilerParams(vmem_limit_bytes=58 * MIB),
    )(got, rows_in)
    back = (2, levels, band_rows, tile_cols)
    return (tracers.reshape(back), velocity.reshape(back), sea_level)


def solution(mesh):
    return jax.shard_map(
        body,
        mesh=mesh,
        in_specs=(P(None, None, "lat", "lon"), P(), P(), P(None, "lat", "lon"), P("lat", "lon")),
        out_specs=(P(None, None, "lat", "lon"), P(None, None, "lat", "lon"), P("lat", "lon")),
        check_vma=False,
    )
```

```python
import functools
import math
import numpy as np
import jax
import jax.numpy as jnp
from jax import lax
from jax.experimental import pallas as pl
from jax.experimental.pallas import tpu as pltpu
from jax.sharding import PartitionSpec as P


WAVE = 0.65
SUB = 20
POLE_ROWS = 128
MIB = 1 << 20
RIM = 21
ROWH = 24
SEG = 225
HALF = SEG // 2
FOLD = 128
MROW = 120


def cplx_add(a, b):
    return (a[0] + b[0], (b[1] if a[1] is None else a[1] if b[1] is None else a[1] + b[1]))


def cplx_sub(a, b):
    if b[1] is None:
        im = a[1]
    elif a[1] is None:
        im = -b[1]
    else:
        im = a[1] - b[1]
    return (a[0] - b[0], im)


def conj(a):
    return (a[0], None if a[1] is None else -a[1])


def turn(a, num, den):
    num %= den
    if num == 0:
        return a
    c, s = math.cos(2 * math.pi * num / den), math.sin(2 * math.pi * num / den)
    re, im = a
    if (4 * num) % den == 0:
        q = 4 * num // den
        if q == 1:
            return (jnp.zeros_like(re) if im is None else -im, re)
        if q == 2:
            return (-re, None if im is None else -im)
        return (jnp.zeros_like(re) if im is None else im, -re)
    if im is None:
        return (re * c, re * s)
    if abs(abs(c) - abs(s)) < 1e-12:
        h = abs(c)
        sc, ss = math.copysign(1.0, c), math.copysign(1.0, s)
        x = re if sc > 0 else -re
        y = im if ss > 0 else -im
        x2 = re if ss > 0 else -re
        y2 = im if sc > 0 else -im
        return ((x - y) * h, (x2 + y2) * h)
    return (re * c - im * s, re * s + im * c)


def real_dft(xs):
    n = len(xs)
    if n == 2:
        return [(xs[0] + xs[1], None), (xs[0] - xs[1], None)]
    even, odd = real_dft(xs[0::2]), real_dft(xs[1::2])
    out = [None] * (n // 2 + 1)
    for r in range(n // 4 + 1):
        o = turn(odd[r], -r, n)
        out[r] = cplx_add(even[r], o)
        if r != n // 2 - r:
            out[n // 2 - r] = conj(cplx_sub(even[r], o))
    return out


def real_idft(ys):
    n = 2 * (len(ys) - 1)
    if n == 2:
        return [ys[0][0] + ys[1][0], ys[0][0] - ys[1][0]]
    even, odd = [], []
    for r in range(n // 4 + 1):
        a, b = ys[r], conj(ys[n // 2 - r])
        if r in (0,):
            a, b = (a[0], None), (b[0], None)
        if r == n // 4:
            even.append((a[0] + a[0], None))
            o = turn((a[0] - a[0], a[1] + a[1]), r, n) if False else None
            odd.append((-(a[1] + a[1]), None))
            continue
        even.append(cplx_add(a, b))
        odd.append(turn(cplx_sub(a, b), r, n))
    e, o = real_idft(even), real_idft(odd)
    out = [None] * n
    out[0::2], out[1::2] = e, o
    return out


def fft_tables():
    at = np.concatenate([np.arange(1, HALF + 1), [0]])
    ang = 2.0 * np.pi * ((at[:, None] * at[None, :]) % SEG) / SEG
    w = np.zeros((2, FOLD, 2 * FOLD), np.float32)
    for half in (0, FOLD):
        w[0, : HALF + 1, half : half + HALF + 1] = np.cos(ang) / 60.0
        w[1, : HALF + 1, half : half + HALF + 1] = np.sin(ang) / 60.0
    tw = np.zeros((HALF, 16), np.float32)
    for r in range(1, 9):
        a = 2.0 * np.pi * r * np.arange(1, HALF + 1) / (16 * SEG)
        tw[:, r - 1] = np.cos(a)
        tw[:, r + 7] = np.sin(a)
    return w, tw


def split(x):
    hi = x.astype(jnp.bfloat16)
    lo = (x - hi.astype(jnp.float32)).astype(jnp.bfloat16)
    return hi, lo


def backward(x):
    rows = 7 - lax.broadcasted_iota(jnp.int32, x.shape, 0)
    return jnp.take_along_axis(x, rows, axis=0)


def whereabouts():
    lat, bands = lax.axis_index("lat"), lax.axis_size("lat")
    edge = POLE_ROWS // ROWS
    return (lat < edge) | (lat >= bands - edge), lax.axis_index("lon")


def filter_kernel(*refs, slots):
    xs = refs[:slots]
    cut_ref, wh_ref, wl_ref, tw_ref = refs[slots : 4 + slots]
    y_hbm, y_ref, e_scr, o_scr, out_sem = refs[-5:]
    polar, lon = whereabouts()
    seats, _, lanes = y_ref.shape
    groups = [pl.ds(0, lanes)]

    def load(d, rows):
        return xs[0][d, rows, :] if slots == 1 else xs[d][rows, :]

    def put(d, where=y_ref):
        to = d if slots == 1 else (lon + d) % seats
        return pltpu.make_async_copy(where.at[d], y_hbm.at[to], out_sem.at[d, 0])

    spans = ((0, 56), (176, 104), (400, 50), (56, 120), (280, 120))

    def put_rows(d, j):
        to = d if slots == 1 else (lon + d) % seats
        at = pl.ds(*spans[j])
        return pltpu.make_async_copy(y_ref.at[d, at], y_hbm.at[to, at], out_sem.at[d, j])

    two = 2 * lanes

    if slots == 1:

        @pl.when(jnp.logical_not(polar))
        def _():
            for d in range(seats):
                put(d, xs[0]).start()
            for d in range(seats):
                put(d, xs[0]).wait()

    @pl.when(polar)
    def _():
        e_scr[HALF:, :] = jnp.zeros((FOLD - HALF, 9 * two), jnp.float32)
        o_scr[HALF:, :] = jnp.zeros((FOLD - HALF, 9 * two), jnp.float32)

        def spots(g, r):
            at = r * two + g * 128
            return pl.ds(at, 128), pl.ds(at + lanes, 128)

        def twiddles(tw, r):
            c = jnp.broadcast_to(tw[:, r - 1 : r], (8, 128))
            s = jnp.broadcast_to(tw[:, r + 7 : r + 8], (8, 128))
            return c, s

        def forward(g):
            first = real_dft([load(s // 2, pl.ds(s % 2 * SEG, 1)) for s in range(16)])
            for r in range(9):
                re_at, im_at = spots(g, r)
                e_scr[HALF : HALF + 1, re_at] = first[r][0]
                if first[r][1] is not None:
                    e_scr[HALF : HALF + 1, im_at] = first[r][1]
            for i in range(HALF // 8):
                rows = pl.ds(8 * i, 8)
                tw = tw_ref[rows, :]
                za = real_dft([load(s // 2, pl.ds(s % 2 * SEG + 8 * i + 1, 8)) for s in range(16)])
                far = [
                    backward(load(s // 2, pl.ds(s % 2 * SEG + SEG - 8 - 8 * i, 8)))
                    for s in range(16)
                ]
                zb = real_dft(far[-1:] + far[:-1])
                re_at, im_at = spots(g, 0)
                e_scr[rows, re_at] = za[0][0] + zb[0][0]
                o_scr[rows, re_at] = za[0][0] - zb[0][0]
                for r in range(1, 9):
                    c, s = twiddles(tw, r)
                    (ar, ai), (br, bi) = za[r], zb[r]
                    if r == 8:
                        ure, uim, vre, vim = ar * c, -(ar * s), br * c, br * s
                    else:
                        ure, uim = ar * c + ai * s, ai * c - ar * s
                        vre, vim = br * c - bi * s, bi * c + br * s
                    re_at, im_at = spots(g, r)
                    e_scr[rows, re_at] = ure + vre
                    o_scr[rows, re_at] = ure - vre
                    e_scr[rows, im_at] = uim + vim
                    o_scr[rows, im_at] = uim - vim

        for g in range(lanes // 128):
            forward(g)
        row = lax.broadcasted_iota(jnp.int32, (MROW, lanes), 0)
        k16 = jnp.where(row < HALF, 16 * (row + 1), 0)
        cut = jnp.broadcast_to(cut_ref[...], (MROW, lanes))

        def product(which, x):
            both = jnp.concatenate(split(x), axis=0)
            f = lambda a: jnp.dot(a, both, preferred_element_type=jnp.float32)
            return (f(wh_ref[which]) + f(wl_ref[which]))[:MROW]

        for r in range(9):
            col = pl.ds(r * two, lanes if r == 0 else two)
            p, q = product(0, e_scr[:, col]), product(1, o_scr[:, col])
            pr, qr = p[:, :lanes], q[:, :lanes]
            near = k16 + r <= cut
            far = (k16 - r <= cut) & (row < HALF)
            if r == 0:
                ere = jnp.where(near, jnp.where(row < HALF, pr + pr, pr), 0.0)
                oim = jnp.where(near, -(qr + qr), 0.0)
                e_scr[0:MROW, col] = ere
                o_scr[0:MROW, col] = oim
                p, q = product(0, e_scr[:, col]), product(1, o_scr[:, col])
                e_scr[0:MROW, col] = p - q
                o_scr[0:MROW, col] = p + q
                continue
            pi, qi = p[:, lanes:], q[:, lanes:]
            xr = jnp.where(near, pr + qi, 0.0)
            xi = jnp.where(near, pi - qr, 0.0)
            yr = jnp.where(far, pr - qi, 0.0)
            yi = jnp.where(far, pi + qr, 0.0)
            e_scr[0:MROW, col] = jnp.concatenate([xr + yr, xi + yi], axis=1)
            o_scr[0:MROW, col] = jnp.concatenate([xr - yr, xi - yi], axis=1)
            p, q = product(0, e_scr[:, col]), product(1, o_scr[:, col])
            pr, qr, pi, qi = p[:, :lanes], q[:, :lanes], p[:, lanes:], q[:, lanes:]
            e_scr[0:MROW, col] = jnp.concatenate([pr - qi, pi + qr], axis=1)
            o_scr[0:MROW, col] = jnp.concatenate([pr + qi, pi - qr], axis=1)

        def inverse(g):
            lane = groups[g]
            ws = []
            for r in range(9):
                re_at, im_at = spots(g, r)
                im = None if r in (0, 8) else e_scr[HALF : HALF + 1, im_at]
                ws.append((e_scr[HALF : HALF + 1, re_at], im))
            ys = real_idft(ws)
            for s in range(16):
                y_ref[s // 2, pl.ds(s % 2 * SEG, 1), lane] = ys[s]
            for i in range(HALF // 8):
                if i == HALF // 16:
                    for d in range(seats):
                        for j in (0, 1, 2):
                            put_rows(d, j).start()
                rows = pl.ds(8 * i, 8)
                tw = tw_ref[rows, :]
                re_at, im_at = spots(g, 0)
                wa, wb = [(e_scr[rows, re_at], None)], [(o_scr[rows, re_at], None)]
                for r in range(1, 9):
                    re_at, im_at = spots(g, r)
                    c, s = twiddles(tw, r)
                    ar, ai, br, bi = e_scr[rows, re_at], e_scr[rows, im_at], o_scr[rows, re_at], o_scr[rows, im_at]
                    wa.append((ar * c - ai * s, None if r == 8 else ai * c + ar * s))
                    wb.append((br * c + bi * s, None if r == 8 else bi * c - br * s))
                ya, yb = real_idft(wa), real_idft(wb)
                for s in range(16):
                    y_ref[s // 2, pl.ds(s % 2 * SEG + 8 * i + 1, 8), lane] = ya[s]
                    y_ref[s // 2, pl.ds(s % 2 * SEG + SEG - 8 - 8 * i, 8), lane] = backward(yb[(s + 1) % 16])

        for g in range(lanes // 128):
            inverse(g)
        for d in range(seats):
            for j in (3, 4):
                put_rows(d, j).start()
        for d in range(seats):
            for j in range(5):
                put_rows(d, j).wait()


def filter_call(xs, cut, tables, twist, shape):
    lanes = xs[0].shape[-1]
    seats = shape[0]
    vmem = pl.BlockSpec(memory_space=pltpu.VMEM)
    far = pl.BlockSpec(memory_space=pltpu.HBM)
    dma = pltpu.SemaphoreType.DMA((seats, 5))
    operands = (*xs, cut, *tables, twist)
    return pl.pallas_call(
        functools.partial(filter_kernel, slots=len(xs)),
        out_shape=pltpu.HBM(shape, jnp.float32),
        in_specs=[vmem] * len(operands),
        out_specs=far,
        scratch_shapes=[
            pltpu.VMEM((seats, 2 * SEG, lanes), jnp.float32),
            pltpu.VMEM((FOLD, 9 * 2 * lanes), jnp.float32),
            pltpu.VMEM((FOLD, 9 * 2 * lanes), jnp.float32),
            dma,
        ],
        name="polar_filter",
        compiler_params=pltpu.CompilerParams(vmem_limit_bytes=20 * MIB),
    )(*operands)


ROWS = 64
COLS = 450
LANES = 512
FAR = 112


def lane_ids(rows):
    return lax.broadcasted_iota(jnp.int32, (rows, 128), 1)


def rim_kernel(flow_ref, land_ref, first_ref, last_ref, scr):
    lane = lane_ids(ROWS)
    first = jnp.zeros((ROWS, 128), jnp.float32)
    last = first
    for a in range(4):
        if a < 3:
            scr[:, 0:COLS] = flow_ref[a]
        else:
            scr[:, 0:COLS] = land_ref[...].astype(jnp.float32)
        mine = (lane >= RIM * a) & (lane < RIM * (a + 1))
        first = jnp.where(mine, pltpu.roll(scr[:, 0:128], RIM * a, 1), first)
        turn_by = (RIM * (a + 1) - (COLS - 384)) % 128
        last = jnp.where(mine, pltpu.roll(scr[:, 384:512], turn_by, 1), last)
    first_ref[...] = first
    last_ref[...] = last


def join_kernel(flow_ref, land_ref, east_ref, west_ref, mid_ref, top_ref, low_ref):
    lane = lane_ids(ROWS)
    for a in range(4):
        if a < 3:
            mid_ref[a, :, 0:COLS] = flow_ref[a]
        else:
            mid_ref[a, :, 0:COLS] = land_ref[...].astype(jnp.float32)
        own = mid_ref[a, :, 384:512]
        west = pltpu.roll(west_ref[...], 128 - RIM * (a + 1), 1)
        east = pltpu.roll(east_ref[...], (COLS - 384 - RIM * a) % 128, 1)
        west = jnp.where(lane >= 128 - RIM, west, 0.0)
        east = jnp.where(lane < COLS - 384 + RIM, east, west)
        mid_ref[a, :, 384:512] = jnp.where(lane < COLS - 384, own, east)
        top_ref[a] = mid_ref[a, 0:ROWH]
        low_ref[a] = mid_ref[a, ROWS - ROWH :]


def step_kernel(at_ref, mid_ref, top_ref, low_ref, out_ref, sea_ref, s_scr, e_scr, n_scr, oc_scr, eo_scr, no_scr):
    first_row = at_ref[0] * ROWS - ROWH
    total = at_ref[1]
    for a, scr in enumerate((s_scr, e_scr, n_scr, oc_scr)):
        scr[0:8] = jnp.zeros((8, LANES), jnp.float32)
        scr[8 + FAR :] = jnp.zeros((8, LANES), jnp.float32)
        scr[8 : 8 + ROWH] = top_ref[a]
        scr[8 + ROWH : 8 + ROWH + ROWS] = mid_ref[a]
        scr[8 + ROWH + ROWS : 8 + FAR] = low_ref[a]
    for b in range(FAR // 8):
        at = 8 + 8 * b
        oc = oc_scr[at : at + 8]
        row = first_row + 8 * b + lax.broadcasted_iota(jnp.int32, (8, LANES), 0)
        last = (row == total - 1) | (row == -1)
        eo = oc * pltpu.roll(oc, LANES - 1, 1)
        no = jnp.where(last, 0.0, oc * oc_scr[at + 1 : at + 9])
        eo_scr[at : at + 8] = eo
        no_scr[at : at + 8] = no
        e_scr[at : at + 8] = e_scr[at : at + 8] * eo
        n_scr[at : at + 8] = n_scr[at : at + 8] * no

    def step(_, carry):
        for b in range(FAR // 8):
            at = 8 + 8 * b
            e = e_scr[at : at + 8]
            div = e - pltpu.roll(e, 1, 1) + n_scr[at : at + 8] - n_scr[at - 1 : at + 7]
            s_scr[at : at + 8] = s_scr[at : at + 8] - WAVE * oc_scr[at : at + 8] * div
        for b in range(FAR // 8):
            at = 8 + 8 * b
            s = s_scr[at : at + 8]
            e_scr[at : at + 8] = eo_scr[at : at + 8] * (
                e_scr[at : at + 8] - WAVE * (pltpu.roll(s, LANES - 1, 1) - s)
            )
            n_scr[at : at + 8] = no_scr[at : at + 8] * (
                n_scr[at : at + 8] - WAVE * (s_scr[at + 1 : at + 9] - s)
            )
        return carry

    lax.fori_loop(0, SUB, step, 0)
    mine = slice(8 + ROWH, 8 + ROWH + ROWS)
    sea_ref[...] = s_scr[mine, 0:COLS]
    for a, scr in enumerate((e_scr, n_scr, eo_scr, no_scr)):
        out_ref[a] = scr[mine, 0:COLS]


def vm():
    return pl.BlockSpec(memory_space=pltpu.VMEM)


def hbm():
    return pl.BlockSpec(memory_space=pltpu.HBM)


def sm():
    return pl.BlockSpec(memory_space=pltpu.SMEM)


def f32(*dims):
    return jax.ShapeDtypeStruct(dims, jnp.float32)


def barotropic_rims(flow, land, shift):
    first, last = pl.pallas_call(
        rim_kernel,
        out_shape=(f32(ROWS, 128), f32(ROWS, 128)),
        in_specs=[vm(), vm()],
        out_specs=(vm(), vm()),
        scratch_shapes=[pltpu.VMEM((ROWS, LANES), jnp.float32)],
        name="rim_columns",
        compiler_params=pltpu.CompilerParams(vmem_limit_bytes=8 * MIB),
    )(flow, land)
    east = shift(first, "lon", -1)
    west = shift(last, "lon", 1)
    return east, west


def barotropic_steps(flow, land, east, west, lat_index, total_rows, shift):
    mid, top, low = pl.pallas_call(
        join_kernel,
        out_shape=(f32(4, ROWS, LANES), f32(4, ROWH, LANES), f32(4, ROWH, LANES)),
        in_specs=[vm()] * 4,
        out_specs=(vm(), vm(), vm()),
        name="join_columns",
        compiler_params=pltpu.CompilerParams(vmem_limit_bytes=8 * MIB),
    )(flow, land, east, west)
    above = shift(low, "lat", 1)
    below = shift(top, "lat", -1)
    where = jnp.stack([lat_index, jnp.int32(total_rows)])
    return pl.pallas_call(
        step_kernel,
        out_shape=(f32(4, ROWS, COLS), f32(ROWS, COLS)),
        in_specs=[sm()] + [vm()] * 3,
        out_specs=(vm(), vm()),
        scratch_shapes=[pltpu.VMEM((FAR + 16, LANES), jnp.float32)] * 6,
        name="subcycles",
        compiler_params=pltpu.CompilerParams(vmem_limit_bytes=8 * MIB),
    )(where, mid, above, below)


def pack_flow_kernel(thick_ref, x_hbm, out_hbm, x_scr, y_scr, in_sem, out_sem):
    parts = out_hbm.shape[0]
    levels = thick_ref.shape[0]
    skip = x_hbm.shape[0] // 2
    per = skip // parts
    gets, puts = [], []
    for p in range(parts):
        span = pl.ds(skip + p * per, per)
        gets.append(pltpu.make_async_copy(x_hbm.at[span], x_scr.at[pl.ds(p * per, per)], in_sem.at[p]))
        gets[-1].start()
    whole = thick_ref[0]
    for k in range(1, levels):
        whole = whole + thick_ref[k]
    scale = 1.0 / jnp.full((1, COLS), whole, jnp.float32)
    group = levels // per
    for p in range(0, parts, group):
        for q in range(group):
            gets[p + q].wait()
        mean = thick_ref[0] * x_scr[p * per]
        for k in range(1, levels):
            mean = mean + thick_ref[k] * x_scr[p * per + k]
        mean = mean * scale
        for q in range(p, p + group):
            y_scr[q] = jnp.concatenate([x_scr[q * per + i] - mean for i in range(per)], axis=0).T
            puts.append(pltpu.make_async_copy(y_scr.at[q], out_hbm.at[q], out_sem.at[q]))
            puts[-1].start()
    for copy in puts:
        copy.wait()


def pack_tracer_kernel(x_hbm, *refs):
    parts = len(refs) - 4
    outs = refs[:parts]
    x_scr, y_scr, in_sem, out_sem = refs[parts:]
    per = x_scr.shape[1]
    polar, lon = whereabouts()

    @pl.when(polar)
    def _():
        gets, puts = [], []
        for k in range(parts):
            span = pl.ds((lon + parts - k) % parts * per, per)
            gets.append(pltpu.make_async_copy(x_hbm.at[span], x_scr.at[k], in_sem.at[k]))
            gets[-1].start()
        for k in range(parts):
            gets[k].wait()
            y_scr[k] = jnp.concatenate([x_scr[k, i] for i in range(per)], axis=0).T
            puts.append(pltpu.make_async_copy(y_scr.at[k], outs[k], out_sem.at[k]))
            puts[-1].start()
        for copy in puts:
            copy.wait()


def unpack_flow_kernel(got_ref, new_ref, speed_hbm, v_scr, v_sem):
    parts = got_ref.shape[0]
    per = speed_hbm.shape[0] // parts
    puts = []
    for p in range(parts):
        field = p // (parts // 2)
        block = got_ref[p].T
        for k in range(per):
            piece = block[k * ROWS : (k + 1) * ROWS]
            v_scr[p, k] = new_ref[2 + field] * (piece + new_ref[field])
        puts.append(pltpu.make_async_copy(v_scr.at[p], speed_hbm.at[pl.ds(p * per, per)], v_sem.at[p]))
        puts[-1].start()
    for copy in puts:
        copy.wait()


def unpack_tracer_kernel(got_hbm, x_hbm, tracer_hbm, got_scr, t_scr, in_sem, out_sem):
    parts = got_hbm.shape[0]
    per = tracer_hbm.shape[0] // parts
    polar, _ = whereabouts()

    def get(p):
        return pltpu.make_async_copy(got_hbm.at[p], got_scr.at[p], in_sem.at[p])

    def keep(p):
        return pltpu.make_async_copy(x_hbm.at[pl.ds(p * per, per)], t_scr.at[p], in_sem.at[p])

    def put(p):
        return pltpu.make_async_copy(t_scr.at[p], tracer_hbm.at[pl.ds(p * per, per)], out_sem.at[p])

    @pl.when(polar)
    def _():
        for p in range(parts):
            get(p).start()
        for p in range(parts):
            get(p).wait()
            block = got_scr[p].T
            for k in range(per):
                t_scr[p, k] = block[k * ROWS : (k + 1) * ROWS]
            put(p).start()

    @pl.when(jnp.logical_not(polar))
    def _():
        for p in range(parts):
            keep(p).start()
        for p in range(parts):
            keep(p).wait()
            put(p).start()

    for p in range(parts):
        put(p).wait()


def shift(value, axis, by):
    size = lax.axis_size(axis)
    return lax.ppermute(value, axis, [(i, (i + by) % size) for i in range(size)])


def body(fields, thickness, cutoff, barotropic, land_sea):
    lon_count = lax.axis_size("lon")
    lat_count = lax.axis_size("lat")
    lat = lax.axis_index("lat")
    components, levels, band_rows, tile_cols = fields.shape
    total_rows = band_rows * lat_count
    pole_rows = cutoff.shape[0] // 2
    pole_bands = pole_rows // band_rows
    bands = [b for b in range(lat_count) if b < pole_bands or b >= lat_count - pole_bands]
    table, twist = fft_tables()
    tables = split(jnp.asarray(table))
    twist = jnp.asarray(twist)
    at = jnp.where(lat < pole_bands, lat * band_rows, lat * band_rows - (total_rows - 2 * pole_rows))
    cuts = lax.dynamic_slice_in_dim(cutoff, jnp.clip(at, 0, 2 * pole_rows - band_rows), band_rows)
    pairs = components * levels
    per = pairs // 2 // lon_count
    half = per * band_rows
    cuts = jnp.tile(cuts, per)[None, :]
    dma = pltpu.SemaphoreType.DMA((lon_count,))
    seats = range(lon_count)
    rows_in = fields.reshape(pairs, band_rows, tile_cols)
    parts = pl.pallas_call(
        pack_flow_kernel,
        out_shape=pltpu.HBM((lon_count, tile_cols, half), jnp.float32),
        in_specs=[sm(), hbm()],
        out_specs=hbm(),
        scratch_shapes=[
            pltpu.VMEM((pairs // 2, band_rows, tile_cols), jnp.float32),
            pltpu.VMEM((lon_count, tile_cols, half), jnp.float32),
            dma,
            dma,
        ],
        name="pack_flow",
        compiler_params=pltpu.CompilerParams(vmem_limit_bytes=60 * MIB),
    )(thickness, rows_in)
    parts = lax.all_to_all(parts, "lon", split_axis=0, concat_axis=0)
    slots = pl.pallas_call(
        pack_tracer_kernel,
        out_shape=[pltpu.HBM((tile_cols, half), jnp.float32) for _ in seats],
        in_specs=[hbm()],
        out_specs=[hbm() for _ in seats],
        scratch_shapes=[
            pltpu.VMEM((lon_count, per, band_rows, tile_cols), jnp.float32),
            pltpu.VMEM((lon_count, tile_cols, half), jnp.float32),
            dma,
            dma,
        ],
        name="pack_tracers",
        compiler_params=pltpu.CompilerParams(vmem_limit_bytes=60 * MIB),
    )(rows_in)
    got = [slots[0]]
    for k in range(1, lon_count):
        route = [
            (i * lat_count + b, (i + lon_count - k) % lon_count * lat_count + b) for b in bands for i in seats
        ]
        got.append(lax.ppermute(slots[k], ("lon", "lat"), route))
    shape = (lon_count, tile_cols, half)
    parts = filter_call([parts], cuts, tables, twist, shape)
    parts = lax.all_to_all(parts, "lon", split_axis=0, concat_axis=0)
    east, west = barotropic_rims(barotropic, land_sea, shift)
    got = filter_call(got, cuts, tables, twist, shape)
    got = lax.all_to_all(got, "lon", split_axis=0, concat_axis=0)
    new, sea_level = barotropic_steps(barotropic, land_sea, east, west, lat, total_rows, shift)
    out = pltpu.HBM((pairs // 2, band_rows, tile_cols), jnp.float32)
    rows_scr = pltpu.VMEM((lon_count, per, band_rows, tile_cols), jnp.float32)
    velocity = pl.pallas_call(
        unpack_flow_kernel,
        out_shape=out,
        in_specs=[vm(), vm()],
        out_specs=hbm(),
        scratch_shapes=[rows_scr, dma],
        name="unpack_flow",
        compiler_params=pltpu.CompilerParams(vmem_limit_bytes=16 * MIB),
    )(parts, new)
    tracers = pl.pallas_call(
        unpack_tracer_kernel,
        out_shape=out,
        in_specs=[hbm(), hbm()],
        out_specs=hbm(),
        scratch_shapes=[pltpu.VMEM(shape, jnp.float32), rows_scr, dma, dma],
        name="unpack_tracers",
        compiler_params=pltpu.CompilerParams(vmem_limit_bytes=58 * MIB),
    )(got, rows_in)
    back = (2, levels, band_rows, tile_cols)
    return (tracers.reshape(back), velocity.reshape(back), sea_level)


def solution(mesh):
    return jax.shard_map(
        body,
        mesh=mesh,
        in_specs=(P(None, None, "lat", "lon"), P(), P(), P(None, "lat", "lon"), P("lat", "lon")),
        out_specs=(P(None, None, "lat", "lon"), P(None, None, "lat", "lon"), P("lat", "lon")),
        check_vma=False,
    )
```
